32 devices in a mesh: win: 8 (over z, x), fsdp: 4 (over y, core).
Axes of the slice: x: 2, y: 2, z: 4, core: 2. Of those that a mesh axis runs over, the one named last changes fastest.
Arguments:
- queries: bfloat16 [8192, 2560], P(('win', 'fsdp')), may hold values from -5 to 5
- keys: bfloat16 [8192, 2560], P(('win', 'fsdp')), may hold values from -5 to 5
- values: bfloat16 [8192, 2560], P(('win', 'fsdp')), may hold values from -6 to 6
- stream: bfloat16 [8192, 5120], P(('win', 'fsdp')), may hold values from -0.59765625 to 0.59765625
- out_weight: bfloat16 [2560, 5120], P('fsdp', 'win'), may hold values from -0.125 to 0.125
- gate: float32 [5120], replicated, may hold values from 0.5 to 2
- head_shift: float32 [5120], replicated, may hold values from -3 to 3
- head_scale: float32 [5120], replicated, may hold values from 0.25 to 1.75
- head_weight: bfloat16 [5120, 64], replicated, may hold values from -0.078125 to 0.078125
- latents: float32 [128, 4096], P('win', 'fsdp'), may hold values from -6 to 6
- step_size: float32 [1], replicated, may hold values from 0.5 to 1
- intersections: int32 [8], replicated, may hold values from 1 to 4
- ramps: int32 [8, 4, 2], replicated, may hold values from 1 to 16
Outputs:
- blended: float32 [128, 4096], P('win', 'fsdp')
The draws below stay inside these ranges and needn't reach their ends.
All inputs are finite; a program needn't handle non-finite values.
Results may differ from the reference program's by a relative error of at most 0.0065.
Values may be sent and summed in bfloat16 or wider, within the bound.
A program may use at most 128 MiB of HBM per device.

```python
import math
import jax
import jax.numpy as jnp
from jax import lax

D = 5120
HEADS = 20
HD = 128
C = 64
P_SIZE = 64
FD = 4
FW = 16
TOKENS = 8192
FRAMES = 128
N_WIN = 8
N_FSDP = 4


def attention_pair(key):
    base = jax.random.fold_in(key, 7)
    first_key, second_key = jax.random.split(base, 2)
    total_rows = N_WIN * FD * N_FSDP * P_SIZE
    columns = HEADS * HD
    query_set = jnp.clip(jax.random.normal(first_key, (total_rows, columns), jnp.float32), -5.0, 5.0)
    key_set = jnp.clip(jax.random.normal(second_key, (total_rows, columns), jnp.float32), -5.0, 5.0)
    return (query_set.astype(jnp.bfloat16), key_set.astype(jnp.bfloat16))


def draw_queries(key, part):
    return attention_pair(key)[0]


def draw_keys(key, part):
    return attention_pair(key)[1]


def set_ends(entries, own_key, least, high):
    dims = entries.shape
    spot = [jax.random.randint(jax.random.fold_in(own_key, axis), (), 0, dims[axis]) for axis in range(len(dims))]
    entries = entries.at[tuple(spot)].set(least)
    longest = dims.index(max(dims))
    spot[longest] = (spot[longest] + 1) % dims[longest]
    return entries.at[tuple(spot)].set(high)


def level_of(stream_key, extent, cuts, least, top_value):
    def one(dim, shards_of):
        steps = jax.random.uniform(jax.random.fold_in(jax.random.fold_in(stream_key, 6), dim), (shards_of,), jnp.float32, least / len(cuts), top_value / len(cuts))
        return jnp.repeat(jnp.exp(steps), extent[dim] // shards_of).reshape((-1,) + (1,) * (len(extent) - dim - 1))

    factor_of = one(*cuts[0])
    for cut in cuts[1:]:
        factor_of = factor_of * one(*cut)
    return factor_of


def noise(own_key, dims, scale, reach, cuts=(), held_as=jnp.bfloat16):
    result = jax.random.normal(own_key, dims, jnp.float32) * scale
    if len(cuts) > 0:
        result = level_of(own_key, dims, cuts, -0.22, 0.18) * result
    return jnp.clip(result, min=-reach, max=reach).astype(held_as)


def setup_inputs(seed: int = 0) -> dict:
    key_list = jax.random.split(jax.random.key(seed), 14)
    queries = draw_queries(jax.random.fold_in(key_list[13], 71), 0)
    keys = draw_keys(jax.random.fold_in(key_list[13], 71), 0)
    values = noise(key_list[2], (TOKENS, HEADS * HD), 1.0, 6.0, ((0, 32),))
    stream = noise(key_list[3], (TOKENS, D), 0.1, 0.59765625, ((0, 32),))
    out_weight = noise(key_list[4], (HEADS * HD, D), (HEADS * HD) ** -0.5, 0.125, ((0, 4), (1, 8)))
    gate = jnp.clip(jax.random.uniform(key_list[5], (D,), jnp.float32, 0.5, 2.0), 0.5, 2.0)
    head_shift = noise(key_list[6], (D,), 0.5, 3.0, (), jnp.float32)
    head_scale = jnp.clip(1.0 + 0.15 * jax.random.normal(key_list[7], (D,), jnp.float32), 0.25, 1.75)
    head_weight = noise(key_list[8], (D, C), D ** -0.5, 0.078125)
    latents = noise(key_list[9], (FRAMES, P_SIZE * C), 1.0, 6.0, ((0, 8), (1, 4)), jnp.float32)
    step_size = jnp.clip(jax.random.uniform(key_list[10], (1,), jnp.float32, 0.5, 1.0), 0.5, 1.0)
    intersections = set_ends(jax.random.randint(key_list[11], (N_WIN,), 1, FD + 1), jax.random.fold_in(key_list[11], 1), 1, FD).astype(jnp.int32)
    ramps = set_ends(jax.random.randint(key_list[12], (N_WIN, FD, 2), 1, 17), jax.random.fold_in(key_list[12], 1), 1, 16).astype(jnp.int32)
    return {"queries": queries, "keys": keys, "values": values, "stream": stream, "out_weight": out_weight, "gate": gate, "head_shift": head_shift, "head_scale": head_scale, "head_weight": head_weight, "latents": latents, "step_size": step_size, "intersections": intersections, "ramps": ramps}


EPSILON = 0.001

def attend(window_parts):
    query_win, key_win, value_win = window_parts
    window_tokens = FW * P_SIZE
    query_h = query_win.reshape(window_tokens, HEADS, HD).astype(jnp.float32)
    key_h = key_win.reshape(window_tokens, HEADS, HD).astype(jnp.float32)
    value_h = value_win.reshape(window_tokens, HEADS, HD).astype(jnp.float32)
    scores = jnp.einsum('qhd,khd->hqk', query_h, key_h) * (1.0 / math.sqrt(HD))
    highest = lax.optimization_barrier(jnp.max(scores, axis=-1, keepdims=True))
    exponent = jnp.exp(scores - highest)
    denominator = lax.optimization_barrier(jnp.sum(exponent, axis=-1))
    probability = exponent.astype(jnp.bfloat16)
    probability = lax.optimization_barrier(probability).astype(jnp.float32)
    summed = jnp.einsum('hqk,khd->qhd', probability, value_h)
    attended = summed / jnp.transpose(denominator)[:, :, None]
    return attended.reshape(window_tokens, HEADS * HD).astype(jnp.bfloat16)

def reference(queries, keys, values, stream, out_weight, gate, head_shift, head_scale, head_weight, latents, step_size, intersections, ramps):
    window_tokens = FW * P_SIZE
    feat_width = HEADS * HD
    attended = lax.map(attend, (queries.reshape(N_WIN, window_tokens, feat_width), keys.reshape(N_WIN, window_tokens, feat_width), values.reshape(N_WIN, window_tokens, feat_width)))
    attended = attended.reshape(N_WIN * window_tokens, feat_width)
    projected = jnp.dot(attended, out_weight, preferred_element_type=jnp.float32)
    hidden = stream.astype(jnp.float32) + gate * projected
    centre = lax.optimization_barrier(jnp.mean(hidden, axis=-1, keepdims=True))
    centred = hidden - centre
    variance = lax.optimization_barrier(jnp.mean(centred * centred, axis=-1, keepdims=True))
    normed = centred / jnp.sqrt(variance + EPSILON)
    modulated = (normed * head_scale + head_shift).astype(jnp.bfloat16)
    velocity = jnp.dot(modulated, head_weight, preferred_element_type=jnp.float32)
    velocity = velocity.reshape(N_WIN, N_FSDP, FW, P_SIZE // N_FSDP, C)
    velocity = jnp.transpose(velocity, (0, 2, 1, 3, 4)).reshape(N_WIN * FW, P_SIZE * C)
    fresh = latents + step_size[0] * velocity
    frames_all = fresh.reshape(N_WIN, FW, P_SIZE * C)
    frame_ids = jnp.arange(FW, dtype=jnp.int32)
    over_prev = jnp.roll(intersections, 1).astype(jnp.int32)
    over_next = intersections.astype(jnp.int32)
    ramp_prev = jnp.roll(ramps, 1, axis=0).astype(jnp.float32)
    ramp_own = ramps.astype(jnp.float32)
    before_win = jnp.roll(frames_all, 1, axis=0)
    after_win = jnp.roll(frames_all, -1, axis=0)
    source_prev = jnp.clip(FW - over_prev[:, None] + frame_ids[None, :], 0, FW - 1).astype(jnp.int32)
    prev_aligned = jnp.take_along_axis(before_win, source_prev[:, :, None], axis=1)
    inside_prev = frame_ids[None, :] < over_prev[:, None]
    prev_index = jnp.minimum(frame_ids, FD - 1).astype(jnp.int32)
    weight_before = ramp_prev[:, prev_index, 0]
    weight_self = ramp_prev[:, prev_index, 1]
    blend_prev = (weight_before[:, :, None] * prev_aligned + weight_self[:, :, None] * frames_all) / (weight_before + weight_self)[:, :, None]
    shifted = frame_ids[None, :] - (FW - over_next[:, None])
    inside_next = shifted >= 0
    source_next = jnp.clip(shifted, 0, FW - 1).astype(jnp.int32)
    next_aligned = jnp.take_along_axis(after_win, source_next[:, :, None], axis=1)
    next_index = jnp.clip(shifted, 0, FD - 1).astype(jnp.int32)
    weight_mine = jnp.take_along_axis(ramp_own[:, :, 0], next_index, axis=1)
    weight_after = jnp.take_along_axis(ramp_own[:, :, 1], next_index, axis=1)
    blend_next = (weight_mine[:, :, None] * frames_all + weight_after[:, :, None] * next_aligned) / (weight_mine + weight_after)[:, :, None]
    blended = jnp.where(inside_prev[:, :, None], blend_prev, jnp.where(inside_next[:, :, None], blend_next, frames_all))
    return blended.reshape(N_WIN * FW, P_SIZE * C)
```

```python
import functools
import math

import jax
import jax.numpy as jnp
from jax import lax
from jax.experimental import pallas as pl
from jax.experimental.pallas import tpu as pltpu
from jax.sharding import PartitionSpec as P

HEADS = 20
HD = 128
FD = 4
EPSILON = 0.001
MESH = pl.DeviceIdType.MESH
F32 = jnp.float32
BF16 = jnp.bfloat16


def kernel(
    ring, n_blk, q_ref, k_ref, v_ref, stream_ref, ow_ref, gate_hbm, shift_hbm, scale_hbm, wt_hbm,
    lat_hbm, step_ref, inter_ref, ramps_ref, out_ref,
    kv, queries, attended, weights, residual, far_hold, near_hold, side_out, side_in, own_out,
    own_in, cross_out, cross_in, hidden, flat, mine, before, after, head_rows,
    gate_ref, shift_ref, scale_ref, wt_ref, lat_ref,
    kv_send, kv_recv, kv_local, q_send, q_recv, q_local, w_send, w_recv, w_local, res_sem,
    par_sem, side_send, side_recv, own_send, own_recv, cross_send, cross_recv, edge_send,
    edge_recv,
):
    win, n_win = lax.axis_index("win"), lax.axis_size("win")
    me, groups = lax.axis_index("fsdp"), lax.axis_size("fsdp")
    rows = q_ref.shape[0]
    heads = kv.shape[1]
    width = weights.shape[2]
    frames, wide = lat_hbm.shape
    channels, model = wt_hbm.shape
    per_frame = rows // frames
    ends = FD * per_frame
    sizes = (2 * ends, rows - 2 * ends)
    pieces = (
        (0, 0, 0, ends),
        (0, rows - ends, ends, ends),
        (1, ends, 0, rows - 2 * ends),
    )
    chip, core = me // 2, me % 2
    sibling = chip * 2 + (1 - core)
    far_chip = 1 - chip
    far = far_chip * 2 + core
    far_sibling = far_chip * 2 + (1 - core)

    up_win, down_win = lax.rem(win + 1, n_win), lax.rem(win + n_win - 1, n_win)
    half_ring = n_win // 2

    def spot_of(w):
        odd = w % 2
        return (1 - odd) * (w // 2) + odd * (n_win - 1 - w // 2)

    def win_of(spot):
        late = spot // half_ring
        return (1 - late) * (2 * spot) + late * (2 * (n_win - 1 - spot) + 1)

    spot = spot_of(win)
    ring_next = win_of(lax.rem(spot + 1, n_win))
    ring_prev = win_of(lax.rem(spot + n_win - 1, n_win))

    if ring:
        blocks = [win]
        for s in range(1, half_ring):
            blocks.append(win_of(lax.rem(spot - s + n_win, n_win)))
            blocks.append(win_of(lax.rem(spot + s, n_win)))
        blocks.append(win_of(lax.rem(spot + half_ring, n_win)))
    else:
        blocks = [jnp.int32(j) for j in range(n_blk)]

    def columns(j):
        return pl.ds(pl.multiple_of(blocks[j] * width, 128), width)

    def head_columns(device, h):
        return pl.ds(pl.multiple_of((device * heads + h) * HD, HD), HD)

    def spots(device, size, start=0, length=None):
        length = size if length is None else length
        return pl.ds(pl.multiple_of(device * size + start, math.gcd(size, start)), length)

    peers = (far, far_sibling, sibling)
    pair = (k_ref, v_ref)

    def kv_copy(t, h, to, slot, source=None):
        source = me if source is None else source
        return pltpu.make_async_remote_copy(
            src_ref=pair[t].at[:, head_columns(to, h)],
            dst_ref=kv.at[t, h, spots(source, rows), :],
            send_sem=kv_send.at[t, h, slot],
            recv_sem=kv_recv.at[t, h, source],
            device_id={"fsdp": to},
            device_id_type=MESH,
        )

    def kv_own(t, h):
        return pltpu.make_async_copy(
            pair[t].at[:, head_columns(me, h)], kv.at[t, h, spots(me, rows), :], kv_local.at[t, h]
        )

    def q_copy(p, h, to, slot, source=None):
        chunk, first, start, length = pieces[p]
        source = me if source is None else source
        return pltpu.make_async_remote_copy(
            src_ref=q_ref.at[pl.ds(first, length), head_columns(to, h)],
            dst_ref=queries[chunk].at[h, spots(source, sizes[chunk], start, length), :],
            send_sem=q_send.at[p, h, slot],
            recv_sem=q_recv.at[p, h, source],
            device_id={"fsdp": to},
            device_id_type=MESH,
        )

    def q_own(p, h):
        chunk, first, start, length = pieces[p]
        return pltpu.make_async_copy(
            q_ref.at[pl.ds(first, length), head_columns(me, h)],
            queries[chunk].at[h, spots(me, sizes[chunk], start, length), :],
            q_local.at[p, h],
        )

    def weight_copy(src, dst, slot, to):
        return pltpu.make_async_remote_copy(
            src_ref=src, dst_ref=dst, send_sem=w_send.at[slot], recv_sem=w_recv.at[slot],
            device_id={"win": to}, device_id_type=MESH,
        )

    depth_half = weights.shape[1] // 2
    last = n_blk - 1

    def forward_copies(s):
        if s < half_ring:
            up_src = ow_ref if s == 1 else weights.at[2 * s - 3]
            down_src = ow_ref if s == 1 else weights.at[2 * s - 2]
            return (
                weight_copy(up_src, weights.at[2 * s - 1], 2 * s - 2, ring_next),
                weight_copy(down_src, weights.at[2 * s], 2 * s - 1, ring_prev),
            )
        top, low = pl.ds(0, depth_half), pl.ds(depth_half, depth_half)
        return (
            weight_copy(weights.at[2 * s - 3, top], weights.at[last, top], 2 * s - 2, ring_next),
            weight_copy(weights.at[2 * s - 2, low], weights.at[last, low], 2 * s - 1, ring_prev),
        )

    def weight_local(j):
        source = ow_ref if ring else ow_ref.at[:, columns(j)]
        return pltpu.make_async_copy(source, weights.at[j], w_local.at[j])

    def residual_copy(p):
        chunk, first, start, length = pieces[p]
        return pltpu.make_async_copy(
            stream_ref.at[pl.ds(first, length), :],
            residual[chunk].at[pl.ds(start, length), :],
            res_sem.at[p],
        )

    parameters = tuple(
        pltpu.make_async_copy(src, dst, par_sem.at[i])
        for i, (src, dst) in enumerate(
            (
                (scale_hbm, scale_ref),
                (shift_hbm, shift_ref),
                (wt_hbm, wt_ref),
                (gate_hbm, gate_ref),
                (lat_hbm, lat_ref),
            )
        )
    )

    barrier = pltpu.get_barrier_semaphore()
    for peer in peers:
        pl.semaphore_signal(barrier, inc=1, device_id={"fsdp": peer}, device_id_type=MESH)
    greeted = [up_win, down_win] + ([ring_next, ring_prev] if ring else [])
    for other in greeted:
        pl.semaphore_signal(barrier, inc=1, device_id={"win": other}, device_id_type=MESH)
    pl.semaphore_wait(barrier, len(peers) + len(greeted))

    def start_kv(h, carry):
        for t in range(2):
            for slot, peer in enumerate(peers):
                kv_copy(t, h, peer, slot).start()
            kv_own(t, h).start()
        return carry

    def start_q(h, carry, chosen):
        for p in chosen:
            for slot, peer in enumerate(peers):
                q_copy(p, h, peer, slot).start()
            q_own(p, h).start()
        return carry

    lax.fori_loop(0, heads, start_kv, 0)
    if ring:
        for copy in forward_copies(1):
            copy.start()
    lax.fori_loop(0, heads, functools.partial(start_q, chosen=(0, 1)), 0)
    lax.fori_loop(0, heads, functools.partial(start_q, chosen=(2,)), 0)
    for copy in parameters:
        copy.start()
    for j in range(1 if ring else n_blk):
        weight_local(j).start()
    for p in range(len(pieces)):
        residual_copy(p).start()

    for copy in parameters:
        copy.wait()
    head = wt_ref[...].astype(F32)
    for i, vector in enumerate((scale_ref, shift_ref)):
        head_rows[8 * i : 8 * i + 8] = lax.dot_general(
            jnp.broadcast_to(vector[...], (8, model)), head, (((1,), (1,)), ((), ())),
            precision=lax.Precision.HIGHEST, preferred_element_type=F32,
        )

    factor = math.log2(math.e) / math.sqrt(HD)

    def attend(h, c, at_chip):
        at = spots(at_chip, 2 * sizes[c])
        scores = lax.dot_general(
            queries[c][h, at, :], kv[0, h], (((1,), (1,)), ((), ())), preferred_element_type=F32
        )
        highest = jnp.max(scores, axis=-1, keepdims=True)
        exponent = jnp.exp2((scores - highest) * factor)
        denominator = jnp.sum(exponent, axis=-1, keepdims=True)
        summed = jnp.dot(exponent.astype(BF16), kv[1, h], preferred_element_type=F32)
        attended[c][at, pl.ds(pl.multiple_of(h * HD, HD), HD)] = (summed / denominator).astype(
            BF16
        )

    def near_head(h, carry):
        for t in range(2):
            for source in peers:
                kv_copy(t, h, source, 0, source).wait_recv()
            kv_own(t, h).wait()
        for p in range(len(pieces)):
            q_copy(p, h, sibling, 0, sibling).wait_recv()
            q_own(p, h).wait()
        for c in range(2):
            attend(h, c, chip)
        return carry

    def far_head(h, carry, c):
        for p, piece in enumerate(pieces):
            if piece[0] == c:
                for source in (far, far_sibling):
                    q_copy(p, h, source, 0, source).wait_recv()
        attend(h, c, far_chip)
        return carry

    early_heads = (heads * 3 + 4) // 5
    lax.fori_loop(0, early_heads, near_head, 0)
    if ring:
        for copy in forward_copies(1):
            copy.wait_recv()
        for copy in forward_copies(2):
            copy.start()
    lax.fori_loop(early_heads, heads, near_head, 0)
    lax.fori_loop(0, heads, functools.partial(far_head, c=0), 0)

    def part_copy(src, dst, send, recv, c, j, to):
        return pltpu.make_async_remote_copy(
            src_ref=src[c].at[j], dst_ref=dst[c].at[j], send_sem=send.at[c, j],
            recv_sem=recv.at[c, j], device_id={"fsdp": to}, device_id_type=MESH,
        )

    def side_copy(c, j):
        return part_copy(side_out, side_in, side_send, side_recv, c, j, sibling)

    def own_copy(c, j):
        return part_copy(own_out, own_in, own_send, own_recv, c, j, sibling)

    def cross_copy(c, j):
        return part_copy(cross_out, cross_in, cross_send, cross_recv, c, j, far)

    def project(c, j):
        size = sizes[c]
        mine_at, other_at = spots(core, size), spots(1 - core, size)
        far_hold[: 2 * size] = jnp.dot(
            attended[c][spots(far_chip, 2 * size), :], weights[j], preferred_element_type=F32
        )
        side_out[c][j] = far_hold[other_at, :].astype(BF16)
        side_copy(c, j).start()
        near_hold[: 2 * size] = jnp.dot(
            attended[c][spots(chip, 2 * size), :], weights[j], preferred_element_type=F32
        )
        own_out[c][j] = near_hold[other_at, :].astype(BF16)
        own_copy(c, j).start()
        side_copy(c, j).wait_recv()
        cross_out[c][j] = (far_hold[mine_at, :] + side_in[c][j].astype(F32)).astype(BF16)
        cross_copy(c, j).start()
        own_copy(c, j).wait_recv()
        hidden[c][j] = residual[c][:, columns(j)].astype(F32) + gate_ref[:, columns(j)] * (
            near_hold[mine_at, :] + own_in[c][j].astype(F32)
        )

    if ring:
        early = 2 * (half_ring - 2) + 1
        split = min(3, early)
        order = [(0, j) for j in range(early)] + [None] + [(1, j) for j in range(split)]
        order += [(0, j) for j in range(early, n_blk)] + [(1, j) for j in range(split, n_blk)]
    else:
        order = [(0, j) for j in range(n_blk)] + [None] + [(1, j) for j in range(n_blk)]

    for p in range(len(pieces)):
        residual_copy(p).wait()
    held = 1
    for step in order:
        if step is None:
            lax.fori_loop(0, heads, functools.partial(far_head, c=1), 0)
            continue
        c, j = step
        if c == 0 and (not ring or j == 0):
            weight_local(j).wait()
        if ring and (j + 1) // 2 > held:
            held = (j + 1) // 2
            for copy in forward_copies(held):
                copy.wait_recv()
            if held < half_ring:
                for copy in forward_copies(held + 1):
                    copy.start()
        project(c, j)

    state = [dict(raw=None, pivot=None, centres=[], spreads=[]) for _ in range(2)]

    def gather(c, j):
        now = state[c]
        cross_copy(c, j).wait_recv()
        block = hidden[c][j] + gate_ref[:, columns(j)] * cross_in[c][j].astype(F32)
        if now["pivot"] is None:
            now["pivot"] = jnp.sum(block, axis=-1, keepdims=True) * (1.0 / width)
        shifted = block - now["pivot"]
        term = lax.dot_general(
            (shifted * scale_ref[:, columns(j)]).astype(BF16), wt_ref[:, columns(j)],
            (((1,), (1,)), ((), ())), preferred_element_type=F32,
        )
        now["raw"] = term if now["raw"] is None else now["raw"] + term
        centre = jnp.sum(shifted, axis=-1, keepdims=True) * (1.0 / width)
        centred = shifted - centre
        now["centres"].append(centre)
        now["spreads"].append(jnp.sum(centred * centred, axis=-1, keepdims=True))

    step_size = step_ref[0]
    chunk_frames = (2 * FD, frames - 2 * FD)
    index = lax.broadcasted_iota(jnp.int32, (2 * FD, 1), 0)
    first_half = index < FD

    def pick(c, at):
        if c == 0:
            return jnp.where(first_half, lat_ref[: 2 * FD, at], lat_ref[frames - 2 * FD :, at])
        spread_over = pltpu.roll(
            jnp.where(first_half, lat_ref[frames - 2 * FD :, at], lat_ref[: 2 * FD, at]), FD, 0
        )
        return spread_over

    def freshen(c):
        now = state[c]
        mean = functools.reduce(jnp.add, now["centres"]) * (1.0 / n_blk)
        spread = functools.reduce(jnp.add, now["spreads"])
        for centre in now["centres"]:
            spread = spread + width * (centre - mean) * (centre - mean)
        inverse = 1.0 / jnp.sqrt(spread * (1.0 / (width * n_blk)) + EPSILON)
        flat[c][:, :channels] = inverse * (now["raw"] - mean * head_rows[:1]) + head_rows[8:9]
        for p in range(0, per_frame, 2):
            pair_of = jnp.concatenate(
                [
                    flat[c][pl.ds(p + i, chunk_frames[c], stride=per_frame), :][:, :channels]
                    for i in range(2)
                ],
                axis=1,
            )
            at = pl.ds(p * channels, 2 * channels)
            mine[c][:, at] = pick(c, at) + step_size * pair_of

    def edge_copy(dst, slot, to):
        return pltpu.make_async_remote_copy(
            src_ref=mine[0], dst_ref=dst, send_sem=edge_send.at[slot], recv_sem=edge_recv.at[slot],
            device_id={"win": to}, device_id_type=MESH,
        )

    edges = (edge_copy(before, 0, up_win), edge_copy(after, 1, down_win))

    def blend():
        edge = 2 * FD
        over_prev, over_next = inter_ref[down_win], inter_ref[win]
        zero = jnp.zeros((edge, 1), jnp.int32)
        theirs_w, own_w = zero, zero
        for i in range(FD):
            hit = (index == i) & (index < over_prev)
            theirs_w = jnp.where(hit, ramps_ref[2 * i, down_win], theirs_w)
            own_w = jnp.where(hit, ramps_ref[2 * i + 1, down_win], own_w)
            hit = index == edge - over_next + i
            own_w = jnp.where(hit, ramps_ref[2 * i, win], own_w)
            theirs_w = jnp.where(hit, ramps_ref[2 * i + 1, win], theirs_w)
        aligned = jnp.zeros((edge, wide), F32)
        earlier, later = before[...], after[...]
        for o in range(1, FD + 1):
            hit = first_half & ((zero + over_prev) == o)
            aligned = jnp.where(hit, pltpu.roll(earlier, o, 0), aligned)
            hit = jnp.logical_not(first_half) & ((zero + over_next) == o)
            aligned = jnp.where(hit, pltpu.roll(later, edge - o, 0), aligned)
        theirs = theirs_w.astype(F32)
        own = jnp.where(own_w > 0, own_w, 1).astype(F32)
        mine[0][...] = (theirs * aligned + own * mine[0][...]) / (theirs + own)

    steps = [step for step in order if step is not None]
    a_done = max(i for i, step in enumerate(steps) if step[0] == 0)
    for c, j in [step for step in steps[: a_done + 1] if step[0] == 0]:
        gather(c, j)
    freshen(0)
    for copy in edges:
        copy.start()
    b_steps = [step for step in steps if step[0] == 1]
    for c, j in b_steps[:-2]:
        gather(c, j)
    for copy in edges:
        copy.wait()
    blend()
    for c, j in b_steps[-2:]:
        gather(c, j)
    freshen(1)

    turned = pltpu.roll(mine[1][...], FD, 0)
    out_ref[: 2 * FD, :] = jnp.where(first_half, mine[0][...], turned)
    out_ref[frames - 2 * FD :, :] = jnp.where(first_half, turned, mine[0][...])

    def finish_head(h, carry):
        for slot, peer in enumerate(peers):
            for t in range(2):
                kv_copy(t, h, peer, slot).wait_send()
            for p in range(len(pieces)):
                q_copy(p, h, peer, slot).wait_send()
        return carry

    lax.fori_loop(0, heads, finish_head, 0)
    if ring:
        for s in range(1, half_ring + 1):
            for copy in forward_copies(s):
                copy.wait_send()
    for c in range(2):
        for j in range(n_blk):
            side_copy(c, j).wait_send()
            own_copy(c, j).wait_send()
            cross_copy(c, j).wait_send()


def local(
    queries,
    keys,
    values,
    stream,
    out_weight,
    gate,
    head_shift,
    head_scale,
    head_weight,
    latents,
    step_size,
    intersections,
    ramps,
):
    rows, features = queries.shape
    groups, n_win = lax.axis_size("fsdp"), lax.axis_size("win")
    heads = features // HD // groups
    depth, part = out_weight.shape
    model = stream.shape[1]
    ring = part % 128 == 0 and n_win % 2 == 0 and n_win >= 6
    if ring:
        n_blk, width = n_win, part
    else:
        n_blk = 8
        width = model // n_blk
        out_weight = lax.all_gather(out_weight, "win", axis=1, tiled=True)
    frames, wide = latents.shape
    assert frames == 4 * FD
    channels = head_weight.shape[1]
    ends = FD * (rows // frames)
    sizes = (2 * ends, rows - 2 * ends)
    any_spec = pl.BlockSpec(memory_space=pl.ANY)
    vmem = pl.BlockSpec(memory_space=pltpu.VMEM)
    smem = pl.BlockSpec(memory_space=pltpu.SMEM)
    dma = pltpu.SemaphoreType.DMA

    def both(shape, dtype):
        return tuple(pltpu.VMEM(shape(size), dtype) for size in sizes)

    parts = both(lambda size: (n_blk, size, width), BF16)
    hold = pltpu.VMEM((2 * max(sizes), width), F32)
    edge = pltpu.VMEM((2 * FD, wide), F32)
    return pl.pallas_call(
        functools.partial(kernel, ring, n_blk),
        out_shape=jax.ShapeDtypeStruct(latents.shape, latents.dtype),
        in_specs=[any_spec] * 10 + [smem] * 3,
        out_specs=vmem,
        scratch_shapes=[
            pltpu.VMEM((2, heads, groups * rows, HD), BF16),
            both(lambda size: (heads, groups * size, HD), BF16),
            both(lambda size: (groups * size, heads * HD), BF16),
            pltpu.VMEM((n_blk, depth, width), BF16),
            both(lambda size: (size, model), BF16),
            hold, hold,
            parts, parts, parts, parts, parts, parts,
            both(lambda size: (n_blk, size, width), F32),
            both(lambda size: (size, 128), F32),
            (edge, pltpu.VMEM((frames - 2 * FD, wide), F32)),
            edge, edge,
            pltpu.VMEM((16, channels), F32),
            pltpu.VMEM((1, model), F32),
            pltpu.VMEM((1, model), F32),
            pltpu.VMEM((1, model), F32),
            pltpu.VMEM((channels, model), head_weight.dtype),
            pltpu.VMEM((frames, wide), F32),
            dma((2, heads, 3)), dma((2, heads, groups)), dma((2, heads)),
            dma((3, heads, 3)), dma((3, heads, groups)), dma((3, heads)),
            dma((n_blk,)), dma((n_blk,)), dma((n_blk,)), dma((3,)), dma((5,)),
            dma((2, n_blk)), dma((2, n_blk)), dma((2, n_blk)), dma((2, n_blk)),
            dma((2, n_blk)), dma((2, n_blk)), dma((2,)), dma((2,)),
        ],
        compiler_params=pltpu.CompilerParams(
            collective_id=0, has_side_effects=True, vmem_limit_bytes=60 * 1024 * 1024
        ),
    )(
        queries, keys, values, stream, out_weight,
        gate[None, :], head_shift[None, :], head_scale[None, :], head_weight.T, latents,
        step_size, intersections, jnp.transpose(ramps, (1, 2, 0)).reshape(-1, n_win),
    )


def solution(mesh):
    in_specs = (
        P(("win", "fsdp"), None),
        P(("win", "fsdp"), None),
        P(("win", "fsdp"), None),
        P(("win", "fsdp"), None),
        P("fsdp", "win"),
        P(),
        P(),
        P(),
        P(),
        P("win", "fsdp"),
        P(),
        P(),
        P(),
    )
    out_specs = P("win", "fsdp")
    return jax.shard_map(local, mesh=mesh, in_specs=in_specs, out_specs=out_specs, check_vma=False)
```

```python
import functools
import math

import jax
import jax.numpy as jnp
from jax import lax
from jax.experimental import pallas as pl
from jax.experimental.pallas import tpu as pltpu
from jax.sharding import PartitionSpec as P

HEADS = 20
HD = 128
FD = 4
EPSILON = 0.001
MESH = pl.DeviceIdType.MESH
F32 = jnp.float32
BF16 = jnp.bfloat16


def kernel(
    ring, n_blk, q_ref, k_ref, v_ref, stream_ref, ow_ref, gate_hbm, shift_hbm, scale_hbm, wt_hbm,
    lat_hbm, step_hbm, inter_hbm, ramps_hbm, out_hbm,
    kv, queries, attended, weights, residual, far_hold, near_hold, side_out, side_in, own_out,
    own_in, cross_out, cross_in, hidden, flat, mine, before, after, head_rows,
    gate_ref, shift_ref, scale_ref, wt_ref, lat_ref, step_ref, inter_ref, ramps_ref, out_ref,
    kv_send, kv_recv, q_near, q_far, own_sem, w_send, w_recv, w_local, res_sem,
    par_sem, out_sem, side_send, side_recv, own_send, own_recv, cross_send, cross_recv, edge_send,
    edge_recv,
):
    win, n_win = lax.axis_index("win"), lax.axis_size("win")
    me, groups = lax.axis_index("fsdp"), lax.axis_size("fsdp")
    rows = q_ref.shape[0]
    heads = kv.shape[1]
    width = weights.shape[2]
    frames, wide = lat_hbm.shape
    channels, model = wt_hbm.shape
    per_frame = rows // frames
    ends = FD * per_frame
    sizes = (2 * ends, rows - 2 * ends)
    pieces = (
        (0, 0, 0, ends),
        (0, rows - ends, ends, ends),
        (1, ends, 0, rows - 2 * ends),
    )
    chip, core = me // 2, me % 2
    sibling = chip * 2 + (1 - core)
    far_chip = 1 - chip
    far = far_chip * 2 + core
    far_sibling = far_chip * 2 + (1 - core)

    up_win, down_win = lax.rem(win + 1, n_win), lax.rem(win + n_win - 1, n_win)
    half_ring = n_win // 2

    def spot_of(w):
        odd = w % 2
        return (1 - odd) * (w // 2) + odd * (n_win - 1 - w // 2)

    def win_of(spot):
        late = spot // half_ring
        return (1 - late) * (2 * spot) + late * (2 * (n_win - 1 - spot) + 1)

    spot = spot_of(win)
    ring_next = win_of(lax.rem(spot + 1, n_win))
    ring_prev = win_of(lax.rem(spot + n_win - 1, n_win))

    if ring:
        blocks = [win]
        for s in range(1, half_ring):
            blocks.append(win_of(lax.rem(spot - s + n_win, n_win)))
            blocks.append(win_of(lax.rem(spot + s, n_win)))
        blocks.append(win_of(lax.rem(spot + half_ring, n_win)))
    else:
        blocks = [jnp.int32(j) for j in range(n_blk)]

    def columns(j):
        return pl.ds(pl.multiple_of(blocks[j] * width, 128), width)

    def head_columns(device, h):
        return pl.ds(pl.multiple_of((device * heads + h) * HD, HD), HD)

    def spots(device, size, start=0, length=None):
        length = size if length is None else length
        return pl.ds(pl.multiple_of(device * size + start, math.gcd(size, start)), length)

    peers = (far, far_sibling, sibling)
    pair = (k_ref, v_ref)

    def kv_copy(t, h, to, slot):
        return pltpu.make_async_remote_copy(
            src_ref=pair[t].at[:, head_columns(to, h)],
            dst_ref=kv.at[t, h, spots(me, rows), :],
            send_sem=kv_send.at[t, slot],
            recv_sem=kv_recv.at[h],
            device_id={"fsdp": to},
            device_id_type=MESH,
        )

    def kv_own(t, h):
        return pltpu.make_async_copy(
            pair[t].at[:, head_columns(me, h)], kv.at[t, h, spots(me, rows), :], own_sem.at[0]
        )

    def q_copy(p, h, to, slot):
        near = slot == 2
        chunk, first, start, length = pieces[p]
        return pltpu.make_async_remote_copy(
            src_ref=q_ref.at[pl.ds(first, length), head_columns(to, h)],
            dst_ref=queries[chunk].at[h, spots(me, sizes[chunk], start, length), :],
            send_sem=kv_send.at[2, slot],
            recv_sem=q_near.at[0] if near else q_far.at[chunk, h],
            device_id={"fsdp": to},
            device_id_type=MESH,
        )

    def q_own(p, h):
        chunk, first, start, length = pieces[p]
        return pltpu.make_async_copy(
            q_ref.at[pl.ds(first, length), head_columns(me, h)],
            queries[chunk].at[h, spots(me, sizes[chunk], start, length), :],
            own_sem.at[1],
        )

    def weight_copy(src, dst, slot, to):
        return pltpu.make_async_remote_copy(
            src_ref=src, dst_ref=dst, send_sem=w_send.at[0], recv_sem=w_recv.at[slot],
            device_id={"win": to}, device_id_type=MESH,
        )

    depth_half = weights.shape[1] // 2
    last = n_blk - 1

    def forward_copies(s):
        if s < half_ring:
            up_src = ow_ref if s == 1 else weights.at[2 * s - 3]
            down_src = ow_ref if s == 1 else weights.at[2 * s - 2]
            return (
                weight_copy(up_src, weights.at[2 * s - 1], 2 * s - 2, ring_next),
                weight_copy(down_src, weights.at[2 * s], 2 * s - 1, ring_prev),
            )
        top, low = pl.ds(0, depth_half), pl.ds(depth_half, depth_half)
        return (
            weight_copy(weights.at[2 * s - 3, top], weights.at[last, top], 2 * s - 2, ring_next),
            weight_copy(weights.at[2 * s - 2, low], weights.at[last, low], 2 * s - 1, ring_prev),
        )

    def weight_local(j):
        source = ow_ref if ring else ow_ref.at[:, columns(j)]
        return pltpu.make_async_copy(source, weights.at[j], w_local.at[0])

    def residual_copy(p):
        chunk, first, start, length = pieces[p]
        return pltpu.make_async_copy(
            stream_ref.at[pl.ds(first, length), :],
            residual[chunk].at[pl.ds(start, length), :],
            res_sem.at[p],
        )

    parameters = tuple(
        pltpu.make_async_copy(src, dst, par_sem.at[i])
        for i, (src, dst) in enumerate(
            (
                (scale_hbm, scale_ref),
                (shift_hbm, shift_ref),
                (wt_hbm, wt_ref),
                (gate_hbm, gate_ref),
                (lat_hbm, lat_ref),
                (step_hbm, step_ref),
                (inter_hbm, inter_ref),
                (ramps_hbm, ramps_ref),
            )
        )
    )

    barrier = pltpu.get_barrier_semaphore()
    for peer in peers:
        pl.semaphore_signal(barrier, inc=1, device_id={"fsdp": peer}, device_id_type=MESH)
    greeted = [ring_next, ring_prev] if ring else [up_win, down_win]
    for other in greeted:
        pl.semaphore_signal(barrier, inc=1, device_id={"win": other}, device_id_type=MESH)
    pl.semaphore_wait(barrier, len(peers) + len(greeted))

    def start_kv(h, carry):
        for t in range(2):
            for slot, peer in enumerate(peers):
                kv_copy(t, h, peer, slot).start()
            kv_own(t, h).start()
        return carry

    def start_q(h, carry, chosen):
        for p in chosen:
            for slot, peer in enumerate(peers):
                q_copy(p, h, peer, slot).start()
            q_own(p, h).start()
        return carry

    lax.fori_loop(0, heads, start_kv, 0)
    if ring:
        for copy in forward_copies(1):
            copy.start()
    lax.fori_loop(0, heads, functools.partial(start_q, chosen=(0, 1)), 0)
    lax.fori_loop(0, heads, functools.partial(start_q, chosen=(2,)), 0)
    for copy in parameters:
        copy.start()
    for j in range(1 if ring else n_blk):
        weight_local(j).start()
    for p in range(len(pieces)):
        residual_copy(p).start()

    for copy in parameters:
        copy.wait()
    head = wt_ref[...].astype(F32)
    for i, vector in enumerate((scale_ref, shift_ref)):
        head_rows[8 * i : 8 * i + 8] = lax.dot_general(
            jnp.broadcast_to(vector[...], (8, model)), head, (((1,), (1,)), ((), ())),
            precision=lax.Precision.HIGHEST, preferred_element_type=F32,
        )

    factor = math.log2(math.e) / math.sqrt(HD)

    def await_bytes(like, sem):
        pltpu.make_async_copy(like, like, sem).wait()

    def attend(h, c, at_chip):
        at = spots(at_chip, 2 * sizes[c])
        scores = lax.dot_general(
            queries[c][h, at, :], kv[0, h], (((1,), (1,)), ((), ())), preferred_element_type=F32
        )
        highest = jnp.max(scores, axis=-1, keepdims=True)
        exponent = jnp.exp2((scores - highest) * factor)
        denominator = jnp.sum(exponent, axis=-1, keepdims=True)
        summed = jnp.dot(exponent.astype(BF16), kv[1, h], preferred_element_type=F32)
        attended[c][at, pl.ds(pl.multiple_of(h * HD, HD), HD)] = (summed / denominator).astype(
            BF16
        )

    def near_head(h, carry):
        await_bytes(kv.at[:, h, pl.ds(0, len(peers) * rows), :], kv_recv.at[h])
        for c in range(2):
            attend(h, c, chip)
        return carry

    def far_head(h, carry, c):
        await_bytes(queries[c].at[h, spots(far_chip, 2 * sizes[c]), :], q_far.at[c, h])
        attend(h, c, far_chip)
        return carry

    own_part = pl.ds(0, rows)
    await_bytes(kv.at[:, :, own_part, :], own_sem.at[0])
    await_bytes(kv.at[0, :, own_part, :], own_sem.at[1])
    await_bytes(kv.at[0, :, own_part, :], q_near.at[0])
    early_heads = (heads * 3 + 4) // 5
    lax.fori_loop(0, early_heads, near_head, 0)
    if ring:
        for copy in forward_copies(1):
            copy.wait_recv()
        for copy in forward_copies(2):
            copy.start()
    lax.fori_loop(early_heads, heads, near_head, 0)
    lax.fori_loop(0, heads, functools.partial(far_head, c=0), 0)

    if ring:
        early = 2 * (half_ring - 2) + 1
        split = min(3, early)
        order = [(0, j) for j in range(early)] + [None] + [(1, j) for j in range(split)]
        order += [(0, j) for j in range(early, n_blk)] + [(1, j) for j in range(split, n_blk)]
    else:
        order = [(0, j) for j in range(n_blk)] + [None] + [(1, j) for j in range(n_blk)]

    steps = [step for step in order if step is not None]
    turn = {step: i for i, step in enumerate(steps)}
    a_steps = [step for step in steps if step[0] == 0]
    b_steps = [step for step in steps if step[0] == 1]
    bins = [a_steps, b_steps[:-3]] + [[step] for step in b_steps[-3:]]
    bin_of = {step: i for i, several in enumerate(bins) for step in several}

    def part_copy(src, dst, send, recv, c, j, to):
        return pltpu.make_async_remote_copy(
            src_ref=src[c].at[j], dst_ref=dst[c].at[j], send_sem=send.at[c], recv_sem=recv,
            device_id={"fsdp": to}, device_id_type=MESH,
        )

    def side_copy(c, j):
        return part_copy(side_out, side_in, side_send, side_recv.at[turn[c, j] % 2], c, j, sibling)

    def own_copy(c, j):
        return part_copy(own_out, own_in, own_send, own_recv.at[turn[c, j] % 2], c, j, sibling)

    def cross_copy(c, j):
        return part_copy(cross_out, cross_in, cross_send, cross_recv.at[bin_of[c, j]], c, j, far)

    def project(c, j):
        size = sizes[c]
        mine_at, other_at = spots(core, size), spots(1 - core, size)
        far_hold[: 2 * size] = jnp.dot(
            attended[c][spots(far_chip, 2 * size), :], weights[j], preferred_element_type=F32
        )
        side_out[c][j] = far_hold[other_at, :].astype(BF16)
        side_copy(c, j).start()
        near_hold[: 2 * size] = jnp.dot(
            attended[c][spots(chip, 2 * size), :], weights[j], preferred_element_type=F32
        )
        own_out[c][j] = near_hold[other_at, :].astype(BF16)
        own_copy(c, j).start()
        side_copy(c, j).wait_recv()
        cross_out[c][j] = (far_hold[mine_at, :] + side_in[c][j].astype(F32)).astype(BF16)
        cross_copy(c, j).start()
        own_copy(c, j).wait_recv()
        hidden[c][j] = residual[c][:, columns(j)].astype(F32) + gate_ref[:, columns(j)] * (
            near_hold[mine_at, :] + own_in[c][j].astype(F32)
        )

    for p in range(len(pieces)):
        residual_copy(p).wait()
    await_bytes(weights.at[: 1 if ring else n_blk], w_local.at[0])
    held = 1
    for step in order:
        if step is None:
            lax.fori_loop(0, heads, functools.partial(far_head, c=1), 0)
            continue
        c, j = step
        if ring and (j + 1) // 2 > held:
            held = (j + 1) // 2
            for copy in forward_copies(held):
                copy.wait_recv()
            if held < half_ring:
                for copy in forward_copies(held + 1):
                    copy.start()
        project(c, j)

    state = [dict(raw=None, pivot=None, centres=[], spreads=[]) for _ in range(2)]

    def gather(c, j):
        now = state[c]
        block = hidden[c][j] + gate_ref[:, columns(j)] * cross_in[c][j].astype(F32)
        if now["pivot"] is None:
            now["pivot"] = jnp.sum(block, axis=-1, keepdims=True) * (1.0 / width)
        shifted = block - now["pivot"]
        term = lax.dot_general(
            (shifted * scale_ref[:, columns(j)]).astype(BF16), wt_ref[:, columns(j)],
            (((1,), (1,)), ((), ())), preferred_element_type=F32,
        )
        now["raw"] = term if now["raw"] is None else now["raw"] + term
        centre = jnp.sum(shifted, axis=-1, keepdims=True) * (1.0 / width)
        centred = shifted - centre
        now["centres"].append(centre)
        now["spreads"].append(jnp.sum(centred * centred, axis=-1, keepdims=True))

    step_size = step_ref[0]
    chunk_frames = (2 * FD, frames - 2 * FD)
    index = lax.broadcasted_iota(jnp.int32, (2 * FD, 1), 0)
    first_half = index < FD

    def pick(c, at):
        if c == 0:
            return jnp.where(first_half, lat_ref[: 2 * FD, at], lat_ref[frames - 2 * FD :, at])
        spread_over = pltpu.roll(
            jnp.where(first_half, lat_ref[frames - 2 * FD :, at], lat_ref[: 2 * FD, at]), FD, 0
        )
        return spread_over

    def freshen(c):
        now = state[c]
        mean = functools.reduce(jnp.add, now["centres"]) * (1.0 / n_blk)
        spread = functools.reduce(jnp.add, now["spreads"])
        for centre in now["centres"]:
            spread = spread + width * (centre - mean) * (centre - mean)
        inverse = 1.0 / jnp.sqrt(spread * (1.0 / (width * n_blk)) + EPSILON)
        flat[c][:, :channels] = inverse * (now["raw"] - mean * head_rows[:1]) + head_rows[8:9]
        for p in range(0, per_frame, 2):
            pair_of = jnp.concatenate(
                [
                    flat[c][pl.ds(p + i, chunk_frames[c], stride=per_frame), :][:, :channels]
                    for i in range(2)
                ],
                axis=1,
            )
            at = pl.ds(p * channels, 2 * channels)
            mine[c][:, at] = pick(c, at) + step_size * pair_of

    def edge_copy(dst, slot, to):
        return pltpu.make_async_remote_copy(
            src_ref=mine[0], dst_ref=dst, send_sem=edge_send.at[slot], recv_sem=edge_recv.at[slot],
            device_id={"win": to}, device_id_type=MESH,
        )

    edges = (edge_copy(before, 0, up_win), edge_copy(after, 1, down_win))

    def blend():
        edge = 2 * FD
        over_prev, over_next = inter_ref[down_win], inter_ref[win]
        zero = jnp.zeros((edge, 1), jnp.int32)
        theirs_w, own_w = zero, zero
        for i in range(FD):
            hit = (index == i) & (index < over_prev)
            theirs_w = jnp.where(hit, ramps_ref[2 * i, down_win], theirs_w)
            own_w = jnp.where(hit, ramps_ref[2 * i + 1, down_win], own_w)
            hit = index == edge - over_next + i
            own_w = jnp.where(hit, ramps_ref[2 * i, win], own_w)
            theirs_w = jnp.where(hit, ramps_ref[2 * i + 1, win], theirs_w)
        aligned = jnp.zeros((edge, wide), F32)
        earlier, later = before[...], after[...]
        for o in range(1, FD + 1):
            hit = first_half & ((zero + over_prev) == o)
            aligned = jnp.where(hit, pltpu.roll(earlier, o, 0), aligned)
            hit = jnp.logical_not(first_half) & ((zero + over_next) == o)
            aligned = jnp.where(hit, pltpu.roll(later, edge - o, 0), aligned)
        theirs = theirs_w.astype(F32)
        own = jnp.where(own_w > 0, own_w, 1).astype(F32)
        mine[0][...] = (theirs * aligned + own * mine[0][...]) / (theirs + own)

    def gather_bin(i):
        c = bins[i][0][0]
        await_bytes(cross_in[c].at[: len(bins[i])], cross_recv.at[i])
        for step in bins[i]:
            gather(*step)

    gather_bin(0)
    freshen(0)
    for copy in edges:
        copy.start()
    gather_bin(1)
    gather_bin(2)
    for copy in edges:
        copy.wait()
    blend()
    gather_bin(3)
    gather_bin(4)
    freshen(1)

    turned = pltpu.roll(mine[1][...], FD, 0)
    out_ref[: 2 * FD, :] = jnp.where(first_half, mine[0][...], turned)
    out_ref[frames - 2 * FD :, :] = jnp.where(first_half, turned, mine[0][...])
    result = pltpu.make_async_copy(out_ref, out_hbm, out_sem.at[0])
    result.start()

    for t in range(3):
        for slot in range(len(peers)):
            await_bytes(kv.at[0, :, own_part, :], kv_send.at[t, slot])
    if ring:
        await_bytes(weights.at[:last], w_send.at[0])
    for c in range(2):
        for send in (side_send, own_send, cross_send):
            await_bytes(cross_in[c], send.at[c])
    result.wait()


def local(
    queries,
    keys,
    values,
    stream,
    out_weight,
    gate,
    head_shift,
    head_scale,
    head_weight,
    latents,
    step_size,
    intersections,
    ramps,
):
    rows, features = queries.shape
    groups, n_win = lax.axis_size("fsdp"), lax.axis_size("win")
    heads = features // HD // groups
    depth, part = out_weight.shape
    model = stream.shape[1]
    ring = part % 128 == 0 and n_win % 2 == 0 and n_win >= 6
    if ring:
        n_blk, width = n_win, part
    else:
        n_blk = 8
        width = model // n_blk
        out_weight = lax.all_gather(out_weight, "win", axis=1, tiled=True)
    frames, wide = latents.shape
    assert frames == 4 * FD
    channels = head_weight.shape[1]
    ends = FD * (rows // frames)
    sizes = (2 * ends, rows - 2 * ends)
    any_spec = pl.BlockSpec(memory_space=pl.ANY)
    dma = pltpu.SemaphoreType.DMA

    def both(shape, dtype):
        return tuple(pltpu.VMEM(shape(size), dtype) for size in sizes)

    parts = both(lambda size: (n_blk, size, width), BF16)
    hold = pltpu.VMEM((2 * max(sizes), width), F32)
    edge = pltpu.VMEM((2 * FD, wide), F32)
    return pl.pallas_call(
        functools.partial(kernel, ring, n_blk),
        out_shape=jax.ShapeDtypeStruct(latents.shape, latents.dtype),
        in_specs=[any_spec] * 13,
        out_specs=any_spec,
        scratch_shapes=[
            pltpu.VMEM((2, heads, groups * rows, HD), BF16),
            both(lambda size: (heads, groups * size, HD), BF16),
            both(lambda size: (groups * size, heads * HD), BF16),
            pltpu.VMEM((n_blk, depth, width), BF16),
            both(lambda size: (size, model), BF16),
            hold, hold,
            parts, parts, parts, parts, parts, parts,
            both(lambda size: (n_blk, size, width), F32),
            both(lambda size: (size, 128), F32),
            (edge, pltpu.VMEM((frames - 2 * FD, wide), F32)),
            edge, edge,
            pltpu.VMEM((16, channels), F32),
            pltpu.VMEM((1, model), F32),
            pltpu.VMEM((1, model), F32),
            pltpu.VMEM((1, model), F32),
            pltpu.VMEM((channels, model), head_weight.dtype),
            pltpu.VMEM((frames, wide), F32),
            pltpu.SMEM((1,), F32),
            pltpu.SMEM((n_win,), jnp.int32),
            pltpu.SMEM((2 * FD, n_win), jnp.int32),
            pltpu.VMEM((frames, wide), F32),
            dma((3, 3)), dma((heads,)), dma((1,)), dma((2, heads)), dma((2,)),
            dma((1,)), dma((n_blk,)), dma((1,)), dma((3,)), dma((8,)), dma((1,)),
            dma((2,)), dma((2,)), dma((2,)), dma((2,)),
            dma((2,)), dma((5,)), dma((2,)), dma((2,)),
        ],
        compiler_params=pltpu.CompilerParams(
            collective_id=0, has_side_effects=True, vmem_limit_bytes=60 * 1024 * 1024
        ),
    )(
        queries, keys, values, stream, out_weight,
        gate[None, :], head_shift[None, :], head_scale[None, :], head_weight.T, latents,
        step_size, intersections, jnp.transpose(ramps, (1, 2, 0)).reshape(-1, n_win),
    )


def solution(mesh):
    in_specs = (
        P(("win", "fsdp"), None),
        P(("win", "fsdp"), None),
        P(("win", "fsdp"), None),
        P(("win", "fsdp"), None),
        P("fsdp", "win"),
        P(),
        P(),
        P(),
        P(),
        P("win", "fsdp"),
        P(),
        P(),
        P(),
    )
    out_specs = P("win", "fsdp")
    return jax.shard_map(local, mesh=mesh, in_specs=in_specs, out_specs=out_specs, check_vma=False)
```

```python
import functools
import math

import jax
import jax.numpy as jnp
from jax import lax
from jax.experimental import pallas as pl
from jax.experimental.pallas import tpu as pltpu
from jax.sharding import PartitionSpec as P

HEADS = 20
HD = 128
FD = 4
EPSILON = 0.001
MESH = pl.DeviceIdType.MESH
F32 = jnp.float32
BF16 = jnp.bfloat16


def kernel(
    ring, n_blk, q_ref, k_ref, v_ref, stream_ref, ow_ref, gate_hbm, shift_hbm, scale_hbm, wt_hbm,
    lat_hbm, step_hbm, inter_hbm, ramps_hbm, out_ref,
    kv, queries, attended, weights, residual, far_hold, near_hold, side_out, side_in, own_out,
    own_in, cross_out, cross_in, hidden, flat, mine, before, after, head_rows,
    gate_ref, shift_ref, scale_ref, wt_ref, lat_ref, step_ref, inter_ref, ramps_ref,
    kv_send, kv_recv, q_near, q_far, own_sem, w_send, w_recv, w_local, res_sem,
    par_sem, side_send, side_recv, own_send, own_recv, cross_send, cross_recv, edge_send,
    edge_recv,
):
    win, n_win = lax.axis_index("win"), lax.axis_size("win")
    me, groups = lax.axis_index("fsdp"), lax.axis_size("fsdp")
    rows = q_ref.shape[0]
    heads = kv.shape[1]
    width = weights.shape[2]
    frames, wide = lat_hbm.shape
    channels, model = wt_hbm.shape
    per_frame = rows // frames
    ends = FD * per_frame
    sizes = (2 * ends, rows - 2 * ends)
    pieces = (
        (0, 0, 0, ends),
        (0, rows - ends, ends, ends),
        (1, ends, 0, rows - 2 * ends),
    )
    chip, core = me // 2, me % 2
    sibling = chip * 2 + (1 - core)
    far_chip = 1 - chip
    far = far_chip * 2 + core
    far_sibling = far_chip * 2 + (1 - core)

    up_win, down_win = lax.rem(win + 1, n_win), lax.rem(win + n_win - 1, n_win)
    half_ring = n_win // 2

    def spot_of(w):
        odd = w % 2
        return (1 - odd) * (w // 2) + odd * (n_win - 1 - w // 2)

    def win_of(spot):
        late = spot // half_ring
        return (1 - late) * (2 * spot) + late * (2 * (n_win - 1 - spot) + 1)

    spot = spot_of(win)
    ring_next = win_of(lax.rem(spot + 1, n_win))
    ring_prev = win_of(lax.rem(spot + n_win - 1, n_win))

    if ring:
        blocks = [win]
        for s in range(1, half_ring):
            blocks.append(win_of(lax.rem(spot - s + n_win, n_win)))
            blocks.append(win_of(lax.rem(spot + s, n_win)))
        blocks.append(win_of(lax.rem(spot + half_ring, n_win)))
    else:
        blocks = [jnp.int32(j) for j in range(n_blk)]

    def columns(j):
        return pl.ds(pl.multiple_of(blocks[j] * width, 128), width)

    def head_columns(device, h):
        return pl.ds(pl.multiple_of((device * heads + h) * HD, HD), HD)

    def spots(device, size, start=0, length=None):
        length = size if length is None else length
        return pl.ds(pl.multiple_of(device * size + start, math.gcd(size, start)), length)

    peers = (far, far_sibling, sibling)
    pair = (k_ref, v_ref)

    def kv_copy(t, h, to, slot):
        return pltpu.make_async_remote_copy(
            src_ref=pair[t].at[:, head_columns(to, h)],
            dst_ref=kv.at[t, h, spots(me, rows), :],
            send_sem=kv_send.at[t, slot],
            recv_sem=kv_recv.at[h],
            device_id={"fsdp": to},
            device_id_type=MESH,
        )

    def kv_own(t, h):
        return pltpu.make_async_copy(
            pair[t].at[:, head_columns(me, h)], kv.at[t, h, spots(me, rows), :], own_sem.at[0]
        )

    def q_copy(p, h, to, slot):
        near = slot == 2
        chunk, first, start, length = pieces[p]
        return pltpu.make_async_remote_copy(
            src_ref=q_ref.at[pl.ds(first, length), head_columns(to, h)],
            dst_ref=queries[chunk].at[h, spots(me, sizes[chunk], start, length), :],
            send_sem=kv_send.at[2, slot],
            recv_sem=q_near.at[0] if near else q_far.at[chunk, h],
            device_id={"fsdp": to},
            device_id_type=MESH,
        )

    def q_own(p, h):
        chunk, first, start, length = pieces[p]
        return pltpu.make_async_copy(
            q_ref.at[pl.ds(first, length), head_columns(me, h)],
            queries[chunk].at[h, spots(me, sizes[chunk], start, length), :],
            own_sem.at[1],
        )

    def weight_copy(src, dst, slot, to):
        return pltpu.make_async_remote_copy(
            src_ref=src, dst_ref=dst, send_sem=w_send.at[0], recv_sem=w_recv.at[slot],
            device_id={"win": to}, device_id_type=MESH,
        )

    depth_half = weights.shape[1] // 2
    last = n_blk - 1

    def forward_copies(s):
        if s < half_ring:
            up_src = ow_ref if s == 1 else weights.at[2 * s - 3]
            down_src = ow_ref if s == 1 else weights.at[2 * s - 2]
            return (
                weight_copy(up_src, weights.at[2 * s - 1], 2 * s - 2, ring_next),
                weight_copy(down_src, weights.at[2 * s], 2 * s - 1, ring_prev),
            )
        top, low = pl.ds(0, depth_half), pl.ds(depth_half, depth_half)
        return (
            weight_copy(weights.at[2 * s - 3, top], weights.at[last, top], 2 * s - 2, ring_next),
            weight_copy(weights.at[2 * s - 2, low], weights.at[last, low], 2 * s - 1, ring_prev),
        )

    def weight_local(j):
        source = ow_ref if ring else ow_ref.at[:, columns(j)]
        return pltpu.make_async_copy(source, weights.at[j], w_local.at[0])

    def residual_copy(p):
        chunk, first, start, length = pieces[p]
        return pltpu.make_async_copy(
            stream_ref.at[pl.ds(first, length), :],
            residual[chunk].at[pl.ds(start, length), :],
            res_sem.at[p],
        )

    parameters = tuple(
        pltpu.make_async_copy(src, dst, par_sem.at[i])
        for i, (src, dst) in enumerate(
            (
                (scale_hbm, scale_ref),
                (shift_hbm, shift_ref),
                (wt_hbm, wt_ref),
                (gate_hbm, gate_ref),
                (lat_hbm, lat_ref),
                (step_hbm, step_ref),
                (inter_hbm, inter_ref),
                (ramps_hbm, ramps_ref),
            )
        )
    )

    barrier = pltpu.get_barrier_semaphore()
    for peer in peers:
        pl.semaphore_signal(barrier, inc=1, device_id={"fsdp": peer}, device_id_type=MESH)
    greeted = [ring_next, ring_prev] if ring else [up_win, down_win]
    for other in greeted:
        pl.semaphore_signal(barrier, inc=1, device_id={"win": other}, device_id_type=MESH)
    pl.semaphore_wait(barrier, len(peers) + len(greeted))

    def start_kv(h, carry):
        for t in range(2):
            for slot, peer in enumerate(peers):
                kv_copy(t, h, peer, slot).start()
            kv_own(t, h).start()
        return carry

    def start_q(h, carry, chosen):
        for p in chosen:
            for slot, peer in enumerate(peers):
                q_copy(p, h, peer, slot).start()
            q_own(p, h).start()
        return carry

    lax.fori_loop(0, heads, start_kv, 0)
    if ring:
        for copy in forward_copies(1):
            copy.start()
    lax.fori_loop(0, heads, functools.partial(start_q, chosen=(0, 1)), 0)
    lax.fori_loop(0, heads, functools.partial(start_q, chosen=(2,)), 0)
    for copy in parameters:
        copy.start()
    for j in range(1 if ring else n_blk):
        weight_local(j).start()
    for p in range(len(pieces)):
        residual_copy(p).start()

    for copy in parameters:
        copy.wait()
    head = wt_ref[...].astype(F32)
    for i, vector in enumerate((scale_ref, shift_ref)):
        head_rows[8 * i : 8 * i + 8] = lax.dot_general(
            jnp.broadcast_to(vector[...], (8, model)), head, (((1,), (1,)), ((), ())),
            precision=lax.Precision.HIGHEST, preferred_element_type=F32,
        )

    factor = math.log2(math.e) / math.sqrt(HD)

    def await_bytes(like, sem):
        pltpu.make_async_copy(like, like, sem).wait()

    def attend(h, c, at_chip):
        at = spots(at_chip, 2 * sizes[c])
        scores = lax.dot_general(
            queries[c][h, at, :], kv[0, h], (((1,), (1,)), ((), ())), preferred_element_type=F32
        )
        highest = jnp.max(scores, axis=-1, keepdims=True)
        exponent = jnp.exp2((scores - highest) * factor)
        denominator = jnp.sum(exponent, axis=-1, keepdims=True)
        summed = jnp.dot(exponent.astype(BF16), kv[1, h], preferred_element_type=F32)
        attended[c][at, pl.ds(pl.multiple_of(h * HD, HD), HD)] = (summed / denominator).astype(
            BF16
        )

    def near_head(h, carry):
        await_bytes(kv.at[:, h, pl.ds(0, len(peers) * rows), :], kv_recv.at[h])
        for c in range(2):
            attend(h, c, chip)
        return carry

    def far_head(h, carry, c):
        await_bytes(queries[c].at[h, spots(far_chip, 2 * sizes[c]), :], q_far.at[c, h])
        attend(h, c, far_chip)
        return carry

    own_part = pl.ds(0, rows)
    await_bytes(kv.at[:, :, own_part, :], own_sem.at[0])
    await_bytes(kv.at[0, :, own_part, :], own_sem.at[1])
    await_bytes(kv.at[0, :, own_part, :], q_near.at[0])
    early_heads = (heads * 3 + 4) // 5
    lax.fori_loop(0, early_heads, near_head, 0)
    if ring:
        for copy in forward_copies(1):
            copy.wait_recv()
        for copy in forward_copies(2):
            copy.start()
    lax.fori_loop(early_heads, heads, near_head, 0)
    lax.fori_loop(0, heads, functools.partial(far_head, c=0), 0)

    if ring:
        early = 2 * (half_ring - 2) + 1
        split = min(3, early)
        order = [(0, j) for j in range(early)] + [None] + [(1, j) for j in range(split)]
        order += [(0, j) for j in range(early, n_blk)] + [(1, j) for j in range(split, n_blk)]
    else:
        order = [(0, j) for j in range(n_blk)] + [None] + [(1, j) for j in range(n_blk)]

    steps = [step for step in order if step is not None]
    turn = {step: i for i, step in enumerate(steps)}
    a_steps = [step for step in steps if step[0] == 0]
    b_steps = [step for step in steps if step[0] == 1]
    bins = [a_steps, b_steps[:-3]] + [[step] for step in b_steps[-3:]]
    bin_of = {step: i for i, several in enumerate(bins) for step in several}

    def part_copy(src, dst, send, recv, c, j, to):
        return pltpu.make_async_remote_copy(
            src_ref=src[c].at[j], dst_ref=dst[c].at[j], send_sem=send.at[c], recv_sem=recv,
            device_id={"fsdp": to}, device_id_type=MESH,
        )

    def side_copy(c, j):
        return part_copy(side_out, side_in, side_send, side_recv.at[turn[c, j] % 2], c, j, sibling)

    def own_copy(c, j):
        return part_copy(own_out, own_in, own_send, own_recv.at[turn[c, j] % 2], c, j, sibling)

    def cross_copy(c, j):
        return part_copy(cross_out, cross_in, cross_send, cross_recv.at[bin_of[c, j]], c, j, far)

    def project(c, j):
        size = sizes[c]
        mine_at, other_at = spots(core, size), spots(1 - core, size)
        far_hold[: 2 * size] = jnp.dot(
            attended[c][spots(far_chip, 2 * size), :], weights[j], preferred_element_type=F32
        )
        side_out[c][j] = far_hold[other_at, :].astype(BF16)
        side_copy(c, j).start()
        near_hold[: 2 * size] = jnp.dot(
            attended[c][spots(chip, 2 * size), :], weights[j], preferred_element_type=F32
        )
        own_out[c][j] = near_hold[other_at, :].astype(BF16)
        own_copy(c, j).start()
        side_copy(c, j).wait_recv()
        cross_out[c][j] = (far_hold[mine_at, :] + side_in[c][j].astype(F32)).astype(BF16)
        cross_copy(c, j).start()
        own_copy(c, j).wait_recv()
        hidden[c][j] = residual[c][:, columns(j)].astype(F32) + gate_ref[:, columns(j)] * (
            near_hold[mine_at, :] + own_in[c][j].astype(F32)
        )

    for p in range(len(pieces)):
        residual_copy(p).wait()
    await_bytes(weights.at[: 1 if ring else n_blk], w_local.at[0])
    held = 1
    for step in order:
        if step is None:
            lax.fori_loop(0, heads, functools.partial(far_head, c=1), 0)
            continue
        c, j = step
        if ring and (j + 1) // 2 > held:
            held = (j + 1) // 2
            for copy in forward_copies(held):
                copy.wait_recv()
            if held < half_ring:
                for copy in forward_copies(held + 1):
                    copy.start()
        project(c, j)

    state = [dict(raw=None, pivot=None, centres=[], spreads=[]) for _ in range(2)]

    def gather(c, j):
        now = state[c]
        block = hidden[c][j] + gate_ref[:, columns(j)] * cross_in[c][j].astype(F32)
        if now["pivot"] is None:
            now["pivot"] = jnp.sum(block, axis=-1, keepdims=True) * (1.0 / width)
        shifted = block - now["pivot"]
        term = lax.dot_general(
            (shifted * scale_ref[:, columns(j)]).astype(BF16), wt_ref[:, columns(j)],
            (((1,), (1,)), ((), ())), preferred_element_type=F32,
        )
        now["raw"] = term if now["raw"] is None else now["raw"] + term
        centre = jnp.sum(shifted, axis=-1, keepdims=True) * (1.0 / width)
        centred = shifted - centre
        now["centres"].append(centre)
        now["spreads"].append(jnp.sum(centred * centred, axis=-1, keepdims=True))

    step_size = step_ref[0]
    chunk_frames = (2 * FD, frames - 2 * FD)
    index = lax.broadcasted_iota(jnp.int32, (2 * FD, 1), 0)
    first_half = index < FD

    def pick(c, at):
        if c == 0:
            return jnp.where(first_half, lat_ref[: 2 * FD, at], lat_ref[frames - 2 * FD :, at])
        spread_over = pltpu.roll(
            jnp.where(first_half, lat_ref[frames - 2 * FD :, at], lat_ref[: 2 * FD, at]), FD, 0
        )
        return spread_over

    def freshen(c):
        now = state[c]
        mean = functools.reduce(jnp.add, now["centres"]) * (1.0 / n_blk)
        spread = functools.reduce(jnp.add, now["spreads"])
        for centre in now["centres"]:
            spread = spread + width * (centre - mean) * (centre - mean)
        inverse = 1.0 / jnp.sqrt(spread * (1.0 / (width * n_blk)) + EPSILON)
        flat[c][:, :channels] = inverse * (now["raw"] - mean * head_rows[:1]) + head_rows[8:9]
        for p in range(0, per_frame, 2):
            pair_of = jnp.concatenate(
                [
                    flat[c][pl.ds(p + i, chunk_frames[c], stride=per_frame), :][:, :channels]
                    for i in range(2)
                ],
                axis=1,
            )
            at = pl.ds(p * channels, 2 * channels)
            mine[c][:, at] = pick(c, at) + step_size * pair_of

    def edge_copy(dst, slot, to):
        return pltpu.make_async_remote_copy(
            src_ref=mine[0], dst_ref=dst, send_sem=edge_send.at[slot], recv_sem=edge_recv.at[slot],
            device_id={"win": to}, device_id_type=MESH,
        )

    edges = (edge_copy(before, 0, up_win), edge_copy(after, 1, down_win))

    def blend():
        edge = 2 * FD
        over_prev, over_next = inter_ref[down_win], inter_ref[win]
        zero = jnp.zeros((edge, 1), jnp.int32)
        theirs_w, own_w = zero, zero
        for i in range(FD):
            hit = (index == i) & (index < over_prev)
            theirs_w = jnp.where(hit, ramps_ref[2 * i, down_win], theirs_w)
            own_w = jnp.where(hit, ramps_ref[2 * i + 1, down_win], own_w)
            hit = index == edge - over_next + i
            own_w = jnp.where(hit, ramps_ref[2 * i, win], own_w)
            theirs_w = jnp.where(hit, ramps_ref[2 * i + 1, win], theirs_w)
        aligned = jnp.zeros((edge, wide), F32)
        earlier, later = before[...], after[...]
        for o in range(1, FD + 1):
            hit = first_half & ((zero + over_prev) == o)
            aligned = jnp.where(hit, pltpu.roll(earlier, o, 0), aligned)
            hit = jnp.logical_not(first_half) & ((zero + over_next) == o)
            aligned = jnp.where(hit, pltpu.roll(later, edge - o, 0), aligned)
        theirs = theirs_w.astype(F32)
        own = jnp.where(own_w > 0, own_w, 1).astype(F32)
        mine[0][...] = (theirs * aligned + own * mine[0][...]) / (theirs + own)

    def gather_bin(i):
        c = bins[i][0][0]
        await_bytes(cross_in[c].at[: len(bins[i])], cross_recv.at[i])
        for step in bins[i]:
            gather(*step)

    gather_bin(0)
    freshen(0)
    for copy in edges:
        copy.start()
    gather_bin(1)
    gather_bin(2)
    for copy in edges:
        copy.wait()
    blend()
    gather_bin(3)
    gather_bin(4)
    freshen(1)

    turned = pltpu.roll(mine[1][...], FD, 0)
    out_ref[: 2 * FD, :] = jnp.where(first_half, mine[0][...], turned)
    out_ref[frames - 2 * FD :, :] = jnp.where(first_half, turned, mine[0][...])

    for t in range(3):
        for slot in range(len(peers)):
            await_bytes(kv.at[0, :, own_part, :], kv_send.at[t, slot])
    if ring:
        await_bytes(weights.at[:last], w_send.at[0])
    for c in range(2):
        for send in (side_send, own_send, cross_send):
            await_bytes(cross_in[c], send.at[c])


def local(
    queries,
    keys,
    values,
    stream,
    out_weight,
    gate,
    head_shift,
    head_scale,
    head_weight,
    latents,
    step_size,
    intersections,
    ramps,
):
    rows, features = queries.shape
    groups, n_win = lax.axis_size("fsdp"), lax.axis_size("win")
    heads = features // HD // groups
    depth, part = out_weight.shape
    model = stream.shape[1]
    ring = part % 128 == 0 and n_win % 2 == 0 and n_win >= 6
    if ring:
        n_blk, width = n_win, part
    else:
        n_blk = 8
        width = model // n_blk
        out_weight = lax.all_gather(out_weight, "win", axis=1, tiled=True)
    frames, wide = latents.shape
    assert frames == 4 * FD
    channels = head_weight.shape[1]
    ends = FD * (rows // frames)
    sizes = (2 * ends, rows - 2 * ends)
    any_spec = pl.BlockSpec(memory_space=pl.ANY)
    dma = pltpu.SemaphoreType.DMA

    def both(shape, dtype):
        return tuple(pltpu.VMEM(shape(size), dtype) for size in sizes)

    parts = both(lambda size: (n_blk, size, width), BF16)
    hold = pltpu.VMEM((2 * max(sizes), width), F32)
    edge = pltpu.VMEM((2 * FD, wide), F32)
    return pl.pallas_call(
        functools.partial(kernel, ring, n_blk),
        out_shape=pltpu.VMEM(latents.shape, latents.dtype),
        in_specs=[any_spec] * 13,
        out_specs=pl.BlockSpec(memory_space=pltpu.VMEM),
        scratch_shapes=[
            pltpu.VMEM((2, heads, groups * rows, HD), BF16),
            both(lambda size: (heads, groups * size, HD), BF16),
            both(lambda size: (groups * size, heads * HD), BF16),
            pltpu.VMEM((n_blk, depth, width), BF16),
            both(lambda size: (size, model), BF16),
            hold, hold,
            parts, parts, parts, parts, parts, parts,
            both(lambda size: (n_blk, size, width), F32),
            both(lambda size: (size, 128), F32),
            (edge, pltpu.VMEM((frames - 2 * FD, wide), F32)),
            edge, edge,
            pltpu.VMEM((16, channels), F32),
            pltpu.VMEM((1, model), F32),
            pltpu.VMEM((1, model), F32),
            pltpu.VMEM((1, model), F32),
            pltpu.VMEM((channels, model), head_weight.dtype),
            pltpu.VMEM((frames, wide), F32),
            pltpu.SMEM((1,), F32),
            pltpu.SMEM((n_win,), jnp.int32),
            pltpu.SMEM((2 * FD, n_win), jnp.int32),
            dma((3, 3)), dma((heads,)), dma((1,)), dma((2, heads)), dma((2,)),
            dma((1,)), dma((n_blk,)), dma((1,)), dma((3,)), dma((8,)),
            dma((2,)), dma((2,)), dma((2,)), dma((2,)),
            dma((2,)), dma((5,)), dma((2,)), dma((2,)),
        ],
        compiler_params=pltpu.CompilerParams(
            collective_id=0, has_side_effects=True, vmem_limit_bytes=60 * 1024 * 1024
        ),
    )(
        queries, keys, values, stream, out_weight,
        gate[None, :], head_shift[None, :], head_scale[None, :], head_weight.T, latents,
        step_size, intersections, jnp.transpose(ramps, (1, 2, 0)).reshape(-1, n_win),
    )


def solution(mesh):
    in_specs = (
        P(("win", "fsdp"), None),
        P(("win", "fsdp"), None),
        P(("win", "fsdp"), None),
        P(("win", "fsdp"), None),
        P("fsdp", "win"),
        P(),
        P(),
        P(),
        P(),
        P("win", "fsdp"),
        P(),
        P(),
        P(),
    )
    out_specs = P("win", "fsdp")
    return jax.shard_map(local, mesh=mesh, in_specs=in_specs, out_specs=out_specs, check_vma=False)
```

```python
import functools
import math

import jax
import jax.numpy as jnp
from jax import lax
from jax.experimental import pallas as pl
from jax.experimental.pallas import tpu as pltpu
from jax.sharding import PartitionSpec as P

HEADS = 20
HD = 128
FD = 4
EPSILON = 0.001
MESH = pl.DeviceIdType.MESH
F32 = jnp.float32
BF16 = jnp.bfloat16


def kernel(
    ring, n_blk, q_ref, k_ref, v_ref, stream_ref, ow_ref, gate_hbm, shift_hbm, scale_hbm, wt_hbm,
    lat_hbm, step_hbm, inter_hbm, ramps_hbm, out_ref,
    kv, queries, attended, weights, residual, far_hold, near_hold, side_out, side_in, own_out,
    own_in, cross_out, cross_in, hidden, flat, mine, around, head_rows,
    staged, vectors, wt_ref, lat_ref, step_ref, inter_ref, ramps_ref, stage_sem,
    kv_send, kv_recv, q_far, own_sem, w_send, w_recv, w_local, res_sem,
    par_sem, part_send, side_recv, own_recv, cross_recv, edge_send,
    edge_recv,
):
    win, n_win = lax.axis_index("win"), lax.axis_size("win")
    me, groups = lax.axis_index("fsdp"), lax.axis_size("fsdp")
    rows = q_ref.shape[0]
    heads = kv.shape[1]
    width = weights.shape[2]
    frames, wide = lat_hbm.shape
    channels, model = wt_hbm.shape
    per_frame = rows // frames
    ends = FD * per_frame
    sizes = (2 * ends, rows - 2 * ends)
    pieces = (
        (0, 0, 0, ends),
        (0, rows - ends, ends, ends),
        (1, ends, 0, rows - 2 * ends),
    )
    chip, core = me // 2, me % 2
    sibling = chip * 2 + (1 - core)
    far_chip = 1 - chip
    far = far_chip * 2 + core
    far_sibling = far_chip * 2 + (1 - core)

    up_win, down_win = lax.rem(win + 1, n_win), lax.rem(win + n_win - 1, n_win)
    half_ring = n_win // 2

    def spot_of(w):
        odd = w % 2
        return (1 - odd) * (w // 2) + odd * (n_win - 1 - w // 2)

    def win_of(spot):
        late = spot // half_ring
        return (1 - late) * (2 * spot) + late * (2 * (n_win - 1 - spot) + 1)

    spot = spot_of(win)
    ring_next = win_of(lax.rem(spot + 1, n_win))
    ring_prev = win_of(lax.rem(spot + n_win - 1, n_win))

    if ring:
        blocks = [win]
        for s in range(1, half_ring):
            blocks.append(win_of(lax.rem(spot - s + n_win, n_win)))
            blocks.append(win_of(lax.rem(spot + s, n_win)))
        blocks.append(win_of(lax.rem(spot + half_ring, n_win)))
    else:
        blocks = [jnp.int32(j) for j in range(n_blk)]

    def columns(j):
        return pl.ds(pl.multiple_of(blocks[j] * width, 128), width)

    def head_columns(device, h):
        return pl.ds(pl.multiple_of((device * heads + h) * HD, HD), HD)

    def spots(device, size, start=0, length=None):
        length = size if length is None else length
        return pl.ds(pl.multiple_of(device * size + start, math.gcd(size, start)), length)

    peers = (far, far_sibling, sibling)
    pair = (staged.at[0], staged.at[1])
    scale_ref, shift_ref, gate_ref = (vectors.at[i] for i in range(3))

    def kv_copy(t, h, to, slot):
        return pltpu.make_async_remote_copy(
            src_ref=pair[t].at[:, head_columns(to, h)],
            dst_ref=kv.at[t, h, spots(me, rows), :],
            send_sem=kv_send.at[0],
            recv_sem=kv_recv.at[h],
            device_id={"fsdp": to},
            device_id_type=MESH,
        )

    def kv_own(t, h):
        return pltpu.make_async_copy(
            pair[t].at[:, head_columns(me, h)], kv.at[t, h, spots(me, rows), :], own_sem.at[0]
        )

    def q_copy(p, h, to, slot):
        near = slot == 2
        chunk, first, start, length = pieces[p]
        return pltpu.make_async_remote_copy(
            src_ref=staged.at[2, pl.ds(first, length), head_columns(to, h)],
            dst_ref=queries[chunk].at[h, spots(me, sizes[chunk], start, length), :],
            send_sem=kv_send.at[1],
            recv_sem=own_sem.at[1] if near else q_far.at[h if chunk == 0 else heads],
            device_id={"fsdp": to},
            device_id_type=MESH,
        )

    def q_own(p, h):
        chunk, first, start, length = pieces[p]
        return pltpu.make_async_copy(
            staged.at[2, pl.ds(first, length), head_columns(me, h)],
            queries[chunk].at[h, spots(me, sizes[chunk], start, length), :],
            own_sem.at[1],
        )

    def weight_copy(src, dst, slot, to):
        return pltpu.make_async_remote_copy(
            src_ref=src, dst_ref=dst, send_sem=w_send.at[0], recv_sem=w_recv.at[slot // 2],
            device_id={"win": to}, device_id_type=MESH,
        )

    depth_half = weights.shape[1] // 2
    last = n_blk - 1

    def forward_copies(s):
        if s < half_ring:
            up_src = ow_ref if s == 1 else weights.at[2 * s - 3]
            down_src = ow_ref if s == 1 else weights.at[2 * s - 2]
            return (
                weight_copy(up_src, weights.at[2 * s - 1], 2 * s - 2, ring_next),
                weight_copy(down_src, weights.at[2 * s], 2 * s - 1, ring_prev),
            )
        top, low = pl.ds(0, depth_half), pl.ds(depth_half, depth_half)
        return (
            weight_copy(weights.at[2 * s - 3, top], weights.at[last, top], 2 * s - 2, ring_next),
            weight_copy(weights.at[2 * s - 2, low], weights.at[last, low], 2 * s - 1, ring_prev),
        )

    def await_weights(s):
        some = weights.at[2 * s - 1 : 2 * s + 1] if s < half_ring else weights.at[last:]
        await_bytes(some, w_recv.at[s - 1])

    def weight_local(j):
        source = ow_ref if ring else ow_ref.at[:, columns(j)]
        return pltpu.make_async_copy(source, weights.at[j], w_local.at[0])

    def residual_copy(p):
        chunk, first, start, length = pieces[p]
        return pltpu.make_async_copy(
            stream_ref.at[pl.ds(first, length), :],
            residual[chunk].at[pl.ds(start, length), :],
            res_sem.at[0],
        )

    loads = [
        pltpu.make_async_copy(src, vectors.at[i], par_sem.at[0])
        for i, src in enumerate((scale_hbm, shift_hbm, gate_hbm))
    ]
    others = [
        pltpu.make_async_copy(src, dst, par_sem.at[1 + i])
        for i, (src, dst) in enumerate(
            (
                (wt_hbm, wt_ref),
                (lat_hbm, lat_ref),
                (step_hbm, step_ref),
                (inter_hbm, inter_ref),
                (ramps_hbm, ramps_ref),
            )
        )
    ]

    stages = tuple(
        pltpu.make_async_copy(src, staged.at[i], stage_sem.at[min(i, 1)])
        for i, src in enumerate((k_ref, v_ref, q_ref))
    )
    for copy in stages:
        copy.start()

    def await_bytes(like, sem):
        pltpu.make_async_copy(like, like, sem).wait()

    barrier = pltpu.get_barrier_semaphore()
    for peer in peers:
        pl.semaphore_signal(barrier, inc=1, device_id={"fsdp": peer}, device_id_type=MESH)
    greeted = [ring_next, ring_prev] if ring else [up_win, down_win]
    for other in greeted:
        pl.semaphore_signal(barrier, inc=1, device_id={"win": other}, device_id_type=MESH)
    pl.semaphore_wait(barrier, len(peers) + len(greeted))

    def start_kv(h, carry, t):
        for slot, peer in enumerate(peers):
            kv_copy(t, h, peer, slot).start()
        kv_own(t, h).start()
        return carry

    def start_q(h, carry, chosen):
        for p in chosen:
            for slot, peer in enumerate(peers):
                q_copy(p, h, peer, slot).start()
            q_own(p, h).start()
        return carry

    stages[0].wait()
    lax.fori_loop(0, heads, functools.partial(start_kv, t=0), 0)
    await_bytes(staged.at[1:], stage_sem.at[1])
    lax.fori_loop(0, heads, functools.partial(start_kv, t=1), 0)
    if ring:
        for copy in forward_copies(1):
            copy.start()
    lax.fori_loop(0, heads, functools.partial(start_q, chosen=(0, 1)), 0)
    lax.fori_loop(0, heads, functools.partial(start_q, chosen=(2,)), 0)
    for copy in loads + others:
        copy.start()
    for j in range(1 if ring else n_blk):
        weight_local(j).start()
    for p in range(len(pieces)):
        residual_copy(p).start()

    await_bytes(vectors, par_sem.at[0])
    for copy in others:
        copy.wait()
    head = wt_ref[...].astype(F32)
    for i, vector in enumerate((scale_ref, shift_ref)):
        head_rows[8 * i : 8 * i + 8] = lax.dot_general(
            jnp.broadcast_to(vector[...], (8, model)), head, (((1,), (1,)), ((), ())),
            precision=lax.Precision.HIGHEST, preferred_element_type=F32,
        )

    factor = math.log2(math.e) / math.sqrt(HD)
    def attend(h, c, at_chip):
        at = spots(at_chip, 2 * sizes[c])
        scores = lax.dot_general(
            queries[c][h, at, :], kv[0, h], (((1,), (1,)), ((), ())), preferred_element_type=F32
        )
        highest = jnp.max(scores, axis=-1, keepdims=True)
        exponent = jnp.exp2((scores - highest) * factor)
        denominator = jnp.sum(exponent, axis=-1, keepdims=True)
        summed = jnp.dot(exponent.astype(BF16), kv[1, h], preferred_element_type=F32)
        attended[c][at, pl.ds(pl.multiple_of(h * HD, HD), HD)] = (summed / denominator).astype(
            BF16
        )

    def near_head(h, carry):
        await_bytes(kv.at[:, h, pl.ds(0, len(peers) * rows), :], kv_recv.at[h])
        for c in range(2):
            attend(h, c, chip)
        return carry

    def far_head(h, carry, c):
        if c == 0:
            await_bytes(queries[c].at[h, spots(far_chip, 2 * sizes[c]), :], q_far.at[h])
        attend(h, c, far_chip)
        return carry

    own_part = pl.ds(0, rows)
    await_bytes(kv.at[:, :, own_part, :], own_sem.at[0])
    await_bytes(kv.at[:, :, own_part, :], own_sem.at[1])
    if ring:
        await_weights(1)
        for copy in forward_copies(2):
            copy.start()
    lax.fori_loop(0, heads, near_head, 0)
    lax.fori_loop(0, heads, functools.partial(far_head, c=0), 0)

    if ring:
        early = 2 * (half_ring - 2) + 1
        split = min(3, early)
        order = [(0, j) for j in range(early)] + [None] + [(1, j) for j in range(split)]
        order += [(0, j) for j in range(early, n_blk)] + [(1, j) for j in range(split, n_blk)]
    else:
        order = [(0, j) for j in range(n_blk)] + [None] + [(1, j) for j in range(n_blk)]

    steps = [step for step in order if step is not None]
    turn = {step: i for i, step in enumerate(steps)}
    a_steps = [step for step in steps if step[0] == 0]
    b_steps = [step for step in steps if step[0] == 1]
    bins = [a_steps, b_steps[:-3]] + [[step] for step in b_steps[-3:]]
    bin_of = {step: i for i, several in enumerate(bins) for step in several}

    def part_copy(src, dst, send, recv, c, j, to):
        return pltpu.make_async_remote_copy(
            src_ref=src[c].at[j], dst_ref=dst[c].at[j], send_sem=part_send.at[c, send], recv_sem=recv,
            device_id={"fsdp": to}, device_id_type=MESH,
        )

    def side_copy(c, j):
        return part_copy(side_out, side_in, 0, side_recv.at[turn[c, j] % 2], c, j, sibling)

    def own_copy(c, j):
        return part_copy(own_out, own_in, 0, own_recv.at[turn[c, j] % 2], c, j, sibling)

    def cross_copy(c, j):
        return part_copy(cross_out, cross_in, 1, cross_recv.at[bin_of[c, j]], c, j, far_sibling)

    def project(c, j):
        size = sizes[c]
        mine_at, other_at = spots(core, size), spots(1 - core, size)
        far_hold[: 2 * size] = jnp.dot(
            attended[c][spots(far_chip, 2 * size), :], weights[j], preferred_element_type=F32
        )
        side_out[c][j] = far_hold[mine_at, :].astype(BF16)
        side_copy(c, j).start()
        near_hold[: 2 * size] = jnp.dot(
            attended[c][spots(chip, 2 * size), :], weights[j], preferred_element_type=F32
        )
        own_out[c][j] = near_hold[other_at, :].astype(BF16)
        own_copy(c, j).start()
        side_copy(c, j).wait_recv()
        cross_out[c][j] = (far_hold[other_at, :] + side_in[c][j].astype(F32)).astype(BF16)
        cross_copy(c, j).start()
        own_copy(c, j).wait_recv()
        hidden[c][j] = residual[c][:, columns(j)].astype(F32) + gate_ref[:, columns(j)] * (
            near_hold[mine_at, :] + own_in[c][j].astype(F32)
        )

    await_bytes(stream_ref, res_sem.at[0])
    await_bytes(weights.at[: 1 if ring else n_blk], w_local.at[0])
    held = 1
    for step in order:
        if step is None:
            far_rows = spots(far_chip, 2 * sizes[1])
            await_bytes(queries[1].at[:, far_rows, :], q_far.at[heads])
            lax.fori_loop(0, heads, functools.partial(far_head, c=1), 0)
            continue
        c, j = step
        if ring and (j + 1) // 2 > held:
            held = (j + 1) // 2
            await_weights(held)
            if held < half_ring:
                for copy in forward_copies(held + 1):
                    copy.start()
        project(c, j)

    state = [dict(raw=None, pivot=None, centres=[], spreads=[]) for _ in range(2)]

    def gather(c, j):
        now = state[c]
        block = hidden[c][j] + gate_ref[:, columns(j)] * cross_in[c][j].astype(F32)
        if now["pivot"] is None:
            now["pivot"] = jnp.sum(block, axis=-1, keepdims=True) * (1.0 / width)
        shifted = block - now["pivot"]
        term = lax.dot_general(
            (shifted * scale_ref[:, columns(j)]).astype(BF16), wt_ref[:, columns(j)],
            (((1,), (1,)), ((), ())), preferred_element_type=F32,
        )
        now["raw"] = term if now["raw"] is None else now["raw"] + term
        centre = jnp.sum(shifted, axis=-1, keepdims=True) * (1.0 / width)
        centred = shifted - centre
        now["centres"].append(centre)
        now["spreads"].append(jnp.sum(centred * centred, axis=-1, keepdims=True))

    step_size = step_ref[0]
    chunk_frames = (2 * FD, frames - 2 * FD)
    index = lax.broadcasted_iota(jnp.int32, (2 * FD, 1), 0)
    first_half = index < FD

    def pick(c, at):
        if c == 0:
            return jnp.where(first_half, lat_ref[: 2 * FD, at], lat_ref[frames - 2 * FD :, at])
        spread_over = pltpu.roll(
            jnp.where(first_half, lat_ref[frames - 2 * FD :, at], lat_ref[: 2 * FD, at]), FD, 0
        )
        return spread_over

    def freshen(c):
        now = state[c]
        mean = functools.reduce(jnp.add, now["centres"]) * (1.0 / n_blk)
        spread = functools.reduce(jnp.add, now["spreads"])
        for centre in now["centres"]:
            spread = spread + width * (centre - mean) * (centre - mean)
        inverse = 1.0 / jnp.sqrt(spread * (1.0 / (width * n_blk)) + EPSILON)
        flat[c][:, :channels] = inverse * (now["raw"] - mean * head_rows[:1]) + head_rows[8:9]
        for p in range(0, per_frame, 2):
            pair_of = jnp.concatenate(
                [
                    flat[c][pl.ds(p + i, chunk_frames[c], stride=per_frame), :][:, :channels]
                    for i in range(2)
                ],
                axis=1,
            )
            at = pl.ds(p * channels, 2 * channels)
            mine[c][:, at] = pick(c, at) + step_size * pair_of

    def edge_copy(slot, to):
        return pltpu.make_async_remote_copy(
            src_ref=mine[0], dst_ref=around.at[slot], send_sem=edge_send.at[0],
            recv_sem=edge_recv.at[0],
            device_id={"win": to}, device_id_type=MESH,
        )

    edges = (edge_copy(0, up_win), edge_copy(1, down_win))

    def blend():
        edge = 2 * FD
        over_prev, over_next = inter_ref[down_win], inter_ref[win]
        zero = jnp.zeros((edge, 1), jnp.int32)
        theirs_w, own_w = zero, zero
        for i in range(FD):
            hit = (index == i) & (index < over_prev)
            theirs_w = jnp.where(hit, ramps_ref[2 * i, down_win], theirs_w)
            own_w = jnp.where(hit, ramps_ref[2 * i + 1, down_win], own_w)
            hit = index == edge - over_next + i
            own_w = jnp.where(hit, ramps_ref[2 * i, win], own_w)
            theirs_w = jnp.where(hit, ramps_ref[2 * i + 1, win], theirs_w)
        aligned = jnp.zeros((edge, wide), F32)
        earlier, later = around[0], around[1]
        for o in range(1, FD + 1):
            hit = first_half & ((zero + over_prev) == o)
            aligned = jnp.where(hit, pltpu.roll(earlier, o, 0), aligned)
            hit = jnp.logical_not(first_half) & ((zero + over_next) == o)
            aligned = jnp.where(hit, pltpu.roll(later, edge - o, 0), aligned)
        theirs = theirs_w.astype(F32)
        own = jnp.where(own_w > 0, own_w, 1).astype(F32)
        mine[0][...] = (theirs * aligned + own * mine[0][...]) / (theirs + own)

    def gather_bin(i):
        c = bins[i][0][0]
        await_bytes(cross_in[c].at[: len(bins[i])], cross_recv.at[i])
        for step in bins[i]:
            gather(*step)

    gather_bin(0)
    freshen(0)
    for copy in edges:
        copy.start()
    gather_bin(1)
    gather_bin(2)
    await_bytes(around, edge_send.at[0])
    await_bytes(around, edge_recv.at[0])
    blend()
    gather_bin(3)
    gather_bin(4)
    freshen(1)

    turned = pltpu.roll(mine[1][...], FD, 0)
    out_ref[: 2 * FD, :] = jnp.where(first_half, mine[0][...], turned)
    out_ref[frames - 2 * FD :, :] = jnp.where(first_half, turned, mine[0][...])

    await_bytes(kv.at[:, :, pl.ds(0, len(peers) * rows), :], kv_send.at[0])
    await_bytes(kv.at[0, :, pl.ds(0, len(peers) * rows), :], kv_send.at[1])
    if ring:
        await_bytes(weights.at[:last], w_send.at[0])
    for c in range(2):
        await_bytes(hidden[c], part_send.at[c, 0])
        await_bytes(cross_in[c], part_send.at[c, 1])


def local(
    queries,
    keys,
    values,
    stream,
    out_weight,
    gate,
    head_shift,
    head_scale,
    head_weight,
    latents,
    step_size,
    intersections,
    ramps,
):
    rows, features = queries.shape
    groups, n_win = lax.axis_size("fsdp"), lax.axis_size("win")
    heads = features // HD // groups
    depth, part = out_weight.shape
    model = stream.shape[1]
    ring = part % 128 == 0 and n_win % 2 == 0 and n_win >= 6
    if ring:
        n_blk, width = n_win, part
    else:
        n_blk = 8
        width = model // n_blk
        out_weight = lax.all_gather(out_weight, "win", axis=1, tiled=True)
    frames, wide = latents.shape
    assert frames == 4 * FD
    channels = head_weight.shape[1]
    ends = FD * (rows // frames)
    sizes = (2 * ends, rows - 2 * ends)
    any_spec = pl.BlockSpec(memory_space=pl.ANY)
    dma = pltpu.SemaphoreType.DMA

    def both(shape, dtype):
        return tuple(pltpu.VMEM(shape(size), dtype) for size in sizes)

    parts = both(lambda size: (n_blk, size, width), BF16)
    hold = pltpu.VMEM((2 * max(sizes), width), F32)
    edge = pltpu.VMEM((2 * FD, wide), F32)
    return pl.pallas_call(
        functools.partial(kernel, ring, n_blk),
        out_shape=pltpu.VMEM(latents.shape, latents.dtype),
        in_specs=[any_spec] * 13,
        out_specs=pl.BlockSpec(memory_space=pltpu.VMEM),
        scratch_shapes=[
            pltpu.VMEM((2, heads, groups * rows, HD), BF16),
            both(lambda size: (heads, groups * size, HD), BF16),
            both(lambda size: (groups * size, heads * HD), BF16),
            pltpu.VMEM((n_blk, depth, width), BF16),
            both(lambda size: (size, model), BF16),
            hold, hold,
            parts, parts, parts, parts, parts, parts,
            both(lambda size: (n_blk, size, width), F32),
            both(lambda size: (size, 128), F32),
            (edge, pltpu.VMEM((frames - 2 * FD, wide), F32)),
            pltpu.VMEM((2, 2 * FD, wide), F32),
            pltpu.VMEM((16, channels), F32),
            pltpu.VMEM((3, rows, features), BF16),
            pltpu.VMEM((3, 1, model), F32),
            pltpu.VMEM((channels, model), head_weight.dtype),
            pltpu.VMEM((frames, wide), F32),
            pltpu.SMEM((1,), F32),
            pltpu.SMEM((n_win,), jnp.int32),
            pltpu.SMEM((2 * FD, n_win), jnp.int32),
            dma((2,)), dma((2,)), dma((heads,)), dma((heads + 1,)), dma((2,)),
            dma((1,)), dma((n_blk // 2,)), dma((1,)), dma((1,)), dma((6,)),
            dma((2, 2)), dma((2,)), dma((2,)), dma((5,)), dma((1,)), dma((1,)),
        ],
        compiler_params=pltpu.CompilerParams(
            collective_id=0, has_side_effects=True, vmem_limit_bytes=60 * 1024 * 1024
        ),
    )(
        queries, keys, values, stream, out_weight,
        gate[None, :], head_shift[None, :], head_scale[None, :], head_weight.T, latents,
        step_size, intersections, jnp.transpose(ramps, (1, 2, 0)).reshape(-1, n_win),
    )


def solution(mesh):
    in_specs = (
        P(("win", "fsdp"), None),
        P(("win", "fsdp"), None),
        P(("win", "fsdp"), None),
        P(("win", "fsdp"), None),
        P("fsdp", "win"),
        P(),
        P(),
        P(),
        P(),
        P("win", "fsdp"),
        P(),
        P(),
        P(),
    )
    out_specs = P("win", "fsdp")
    return jax.shard_map(local, mesh=mesh, in_specs=in_specs, out_specs=out_specs, check_vma=False)
```

```python
import functools
import math

import jax
import jax.numpy as jnp
from jax import lax
from jax.experimental import pallas as pl
from jax.experimental.pallas import tpu as pltpu
from jax.sharding import PartitionSpec as P

HEADS = 20
HD = 128
FD = 4
EPSILON = 0.001
MESH = pl.DeviceIdType.MESH
F32 = jnp.float32
BF16 = jnp.bfloat16


def kernel(
    ring, n_blk, q_ref, k_ref, v_ref, stream_ref, ow_ref, gate_hbm, shift_hbm, scale_hbm, wt_hbm,
    lat_hbm, step_hbm, inter_hbm, ramps_hbm, out_ref,
    kv, queries, attended, weights, residual, far_hold, near_hold, side_out, side_in, own_out,
    own_in, cross_out, cross_in, hidden, flat, mine, around, head_rows,
    staged, vectors, wt_ref, lat_ref, step_ref, inter_ref, ramps_ref, stage_sem,
    kv_send, kv_recv, q_far, own_sem, w_send, w_recv, w_local, res_sem,
    par_sem, part_send, side_recv, own_recv, cross_recv, edge_send,
    edge_recv,
):
    win, n_win = lax.axis_index("win"), lax.axis_size("win")
    me, groups = lax.axis_index("fsdp"), lax.axis_size("fsdp")
    rows = q_ref.shape[0]
    heads = kv.shape[1]
    width = weights.shape[2]
    frames, wide = lat_hbm.shape
    channels, model = wt_hbm.shape
    per_frame = rows // frames
    ends = FD * per_frame
    sizes = (2 * ends, rows - 2 * ends)
    pieces = (
        (0, 0, 0, ends),
        (0, rows - ends, ends, ends),
        (1, ends, 0, rows - 2 * ends),
    )
    chip, core = me // 2, me % 2
    sibling = chip * 2 + (1 - core)
    far_chip = 1 - chip
    far = far_chip * 2 + core
    far_sibling = far_chip * 2 + (1 - core)

    up_win, down_win = lax.rem(win + 1, n_win), lax.rem(win + n_win - 1, n_win)
    half_ring = n_win // 2

    def spot_of(w):
        odd = w % 2
        return (1 - odd) * (w // 2) + odd * (n_win - 1 - w // 2)

    def win_of(spot):
        late = spot // half_ring
        return (1 - late) * (2 * spot) + late * (2 * (n_win - 1 - spot) + 1)

    spot = spot_of(win)
    ring_next = win_of(lax.rem(spot + 1, n_win))
    ring_prev = win_of(lax.rem(spot + n_win - 1, n_win))

    if ring:
        blocks = [win]
        for s in range(1, half_ring):
            blocks.append(win_of(lax.rem(spot - s + n_win, n_win)))
            blocks.append(win_of(lax.rem(spot + s, n_win)))
        blocks.append(win_of(lax.rem(spot + half_ring, n_win)))
    else:
        blocks = [jnp.int32(j) for j in range(n_blk)]

    def columns(j):
        return pl.ds(pl.multiple_of(blocks[j] * width, 128), width)

    def head_columns(device, h):
        return pl.ds(pl.multiple_of((device * heads + h) * HD, HD), HD)

    def spots(device, size, start=0, length=None):
        length = size if length is None else length
        return pl.ds(pl.multiple_of(device * size + start, math.gcd(size, start)), length)

    peers = (far, far_sibling, sibling)
    pair = (staged.at[0], staged.at[1])
    scale_ref, shift_ref, gate_ref = (vectors.at[i] for i in range(3))

    def kv_copy(t, h, to, slot):
        return pltpu.make_async_remote_copy(
            src_ref=pair[t].at[:, head_columns(to, h)],
            dst_ref=kv.at[t, h, spots(me, rows), :],
            send_sem=kv_send.at[0],
            recv_sem=kv_recv.at[h],
            device_id={"fsdp": to},
            device_id_type=MESH,
        )

    def kv_own(t, h):
        return pltpu.make_async_copy(
            pair[t].at[:, head_columns(me, h)], kv.at[t, h, spots(me, rows), :], own_sem.at[0]
        )

    def q_copy(p, h, to, slot):
        near = slot == 2
        chunk, first, start, length = pieces[p]
        return pltpu.make_async_remote_copy(
            src_ref=staged.at[2, pl.ds(first, length), head_columns(to, h)],
            dst_ref=queries[chunk].at[h, spots(me, sizes[chunk], start, length), :],
            send_sem=kv_send.at[1],
            recv_sem=own_sem.at[1] if near else q_far.at[h if chunk == 0 else heads],
            device_id={"fsdp": to},
            device_id_type=MESH,
        )

    def q_own(p, h):
        chunk, first, start, length = pieces[p]
        return pltpu.make_async_copy(
            staged.at[2, pl.ds(first, length), head_columns(me, h)],
            queries[chunk].at[h, spots(me, sizes[chunk], start, length), :],
            own_sem.at[1],
        )

    def weight_copy(src, dst, slot, to):
        return pltpu.make_async_remote_copy(
            src_ref=src, dst_ref=dst, send_sem=w_send.at[0], recv_sem=w_recv.at[slot // 2],
            device_id={"win": to}, device_id_type=MESH,
        )

    depth_half = weights.shape[1] // 2
    last = n_blk - 1

    def forward_copies(s):
        if s < half_ring:
            up_src = ow_ref if s == 1 else weights.at[2 * s - 3]
            down_src = ow_ref if s == 1 else weights.at[2 * s - 2]
            return (
                weight_copy(up_src, weights.at[2 * s - 1], 2 * s - 2, ring_next),
                weight_copy(down_src, weights.at[2 * s], 2 * s - 1, ring_prev),
            )
        top, low = pl.ds(0, depth_half), pl.ds(depth_half, depth_half)
        return (
            weight_copy(weights.at[2 * s - 3, top], weights.at[last, top], 2 * s - 2, ring_next),
            weight_copy(weights.at[2 * s - 2, low], weights.at[last, low], 2 * s - 1, ring_prev),
        )

    def await_weights(s):
        some = weights.at[2 * s - 1 : 2 * s + 1] if s < half_ring else weights.at[last:]
        await_bytes(some, w_recv.at[s - 1])

    def weight_local(j):
        source = ow_ref if ring else ow_ref.at[:, columns(j)]
        return pltpu.make_async_copy(source, weights.at[j], w_local.at[0])

    def residual_copy(p):
        chunk, first, start, length = pieces[p]
        return pltpu.make_async_copy(
            stream_ref.at[pl.ds(first, length), :],
            residual[chunk].at[pl.ds(start, length), :],
            res_sem.at[0],
        )

    loads = [
        pltpu.make_async_copy(src, vectors.at[i], par_sem.at[0])
        for i, src in enumerate((scale_hbm, shift_hbm, gate_hbm))
    ]
    others = [
        pltpu.make_async_copy(src, dst, par_sem.at[1 + i])
        for i, (src, dst) in enumerate(
            (
                (wt_hbm, wt_ref),
                (lat_hbm, lat_ref),
                (step_hbm, step_ref),
                (inter_hbm, inter_ref),
                (ramps_hbm, ramps_ref),
            )
        )
    ]

    stages = tuple(
        pltpu.make_async_copy(src, staged.at[i], stage_sem.at[min(i, 1)])
        for i, src in enumerate((k_ref, v_ref, q_ref))
    )
    for copy in stages:
        copy.start()

    def await_bytes(like, sem):
        pltpu.make_async_copy(like, like, sem).wait()

    barrier = pltpu.get_barrier_semaphore()
    for peer in peers:
        pl.semaphore_signal(barrier, inc=1, device_id={"fsdp": peer}, device_id_type=MESH)
    greeted = [ring_next, ring_prev] if ring else [up_win, down_win]
    for other in greeted:
        pl.semaphore_signal(barrier, inc=1, device_id={"win": other}, device_id_type=MESH)
    pl.semaphore_wait(barrier, len(peers) + len(greeted))

    def start_kv(h, carry, t):
        for slot, peer in enumerate(peers):
            kv_copy(t, h, peer, slot).start()
        kv_own(t, h).start()
        return carry

    def start_q(h, carry, chosen):
        for p in chosen:
            for slot, peer in enumerate(peers):
                q_copy(p, h, peer, slot).start()
            q_own(p, h).start()
        return carry

    stages[0].wait()
    lax.fori_loop(0, heads, functools.partial(start_kv, t=0), 0)
    await_bytes(staged.at[1:], stage_sem.at[1])
    lax.fori_loop(0, heads, functools.partial(start_kv, t=1), 0)
    if ring:
        for copy in forward_copies(1):
            copy.start()
    lax.fori_loop(0, heads, functools.partial(start_q, chosen=(0, 1)), 0)
    lax.fori_loop(0, heads, functools.partial(start_q, chosen=(2,)), 0)
    for copy in loads + others:
        copy.start()
    for j in range(1 if ring else n_blk):
        weight_local(j).start()
    for p in range(len(pieces)):
        residual_copy(p).start()

    await_bytes(vectors, par_sem.at[0])
    for copy in others:
        copy.wait()
    head = wt_ref[...].astype(F32)
    for i, vector in enumerate((scale_ref, shift_ref)):
        head_rows[8 * i : 8 * i + 8] = lax.dot_general(
            jnp.broadcast_to(vector[...], (8, model)), head, (((1,), (1,)), ((), ())),
            precision=lax.Precision.HIGHEST, preferred_element_type=F32,
        )

    factor = math.log2(math.e) / math.sqrt(HD)
    def attend(h, c, at_chip):
        at = spots(at_chip, 2 * sizes[c])
        scores = lax.dot_general(
            queries[c][h, at, :], kv[0, h], (((1,), (1,)), ((), ())), preferred_element_type=F32
        )
        highest = jnp.max(scores, axis=-1, keepdims=True)
        exponent = jnp.exp2((scores - highest) * factor)
        denominator = jnp.sum(exponent, axis=-1, keepdims=True)
        summed = jnp.dot(exponent.astype(BF16), kv[1, h], preferred_element_type=F32)
        attended[c][at, pl.ds(pl.multiple_of(h * HD, HD), HD)] = (summed / denominator).astype(
            BF16
        )

    def near_head(h, carry):
        await_bytes(kv.at[:, h, pl.ds(0, len(peers) * rows), :], kv_recv.at[h])
        for c in range(2):
            attend(h, c, chip)
        return carry

    def far_head(h, carry, c):
        if c == 0:
            await_bytes(queries[c].at[h, spots(far_chip, 2 * sizes[c]), :], q_far.at[h])
        attend(h, c, far_chip)
        return carry

    own_part = pl.ds(0, rows)
    await_bytes(kv.at[:, :, own_part, :], own_sem.at[0])
    await_bytes(kv.at[:, :, own_part, :], own_sem.at[1])
    if ring:
        await_weights(1)
        for copy in forward_copies(2):
            copy.start()
    lax.fori_loop(0, heads, near_head, 0)
    lax.fori_loop(0, heads, functools.partial(far_head, c=0), 0)

    if ring:
        early = 2 * (half_ring - 2) + 1
        split = min(3, early)
        order = [(0, j) for j in range(early)] + [None] + [(1, j) for j in range(split)]
        order += [(0, j) for j in range(early, n_blk)] + [(1, j) for j in range(split, n_blk)]
    else:
        order = [(0, j) for j in range(n_blk)] + [None] + [(1, j) for j in range(n_blk)]

    steps = [step for step in order if step is not None]
    turn = {step: i for i, step in enumerate(steps)}
    a_steps = [step for step in steps if step[0] == 0]
    b_steps = [step for step in steps if step[0] == 1]
    bins = [a_steps, b_steps[:-3]] + [[step] for step in b_steps[-3:]]
    bin_of = {step: i for i, several in enumerate(bins) for step in several}

    def part_copy(src, dst, send, recv, c, j, to):
        return pltpu.make_async_remote_copy(
            src_ref=src[c].at[j], dst_ref=dst[c].at[j], send_sem=part_send.at[c, send], recv_sem=recv,
            device_id={"fsdp": to}, device_id_type=MESH,
        )

    def side_copy(c, j):
        return part_copy(side_out, side_in, 0, side_recv.at[turn[c, j] % 2], c, j, sibling)

    def own_copy(c, j):
        return part_copy(own_out, own_in, 0, own_recv.at[turn[c, j] % 2], c, j, sibling)

    def cross_copy(c, j):
        return part_copy(cross_out, cross_in, 1, cross_recv.at[bin_of[c, j]], c, j, far_sibling)

    def project(c, j):
        size = sizes[c]
        mine_at, other_at = spots(core, size), spots(1 - core, size)
        far_hold[: 2 * size] = jnp.dot(
            attended[c][spots(far_chip, 2 * size), :], weights[j], preferred_element_type=F32
        )
        side_out[c][j] = far_hold[mine_at, :].astype(BF16)
        side_copy(c, j).start()
        near_hold[: 2 * size] = jnp.dot(
            attended[c][spots(chip, 2 * size), :], weights[j], preferred_element_type=F32
        )
        own_out[c][j] = near_hold[other_at, :].astype(BF16)
        own_copy(c, j).start()
        side_copy(c, j).wait_recv()
        cross_out[c][j] = (far_hold[other_at, :] + side_in[c][j].astype(F32)).astype(BF16)
        cross_copy(c, j).start()
        own_copy(c, j).wait_recv()
        hidden[c][j] = residual[c][:, columns(j)].astype(F32) + gate_ref[:, columns(j)] * (
            near_hold[mine_at, :] + own_in[c][j].astype(F32)
        )

    await_bytes(stream_ref, res_sem.at[0])
    await_bytes(weights.at[: 1 if ring else n_blk], w_local.at[0])
    held = 1

    def advance():
        nonlocal held
        held += 1
        await_weights(held)
        if held < half_ring:
            for copy in forward_copies(held + 1):
                copy.start()

    for step in order:
        if step is None:
            far_rows = spots(far_chip, 2 * sizes[1])
            await_bytes(queries[1].at[:, far_rows, :], q_far.at[heads])
            lax.fori_loop(0, heads, functools.partial(far_head, c=1), 0)
            continue
        c, j = step
        if ring and (j + 1) // 2 > held:
            advance()
        project(c, j)
        if ring and step == steps[0]:
            advance()

    state = [dict(raw=None, pivot=None, centres=[], spreads=[]) for _ in range(2)]

    def gather(c, j):
        now = state[c]
        block = hidden[c][j] + gate_ref[:, columns(j)] * cross_in[c][j].astype(F32)
        if now["pivot"] is None:
            now["pivot"] = jnp.sum(block, axis=-1, keepdims=True) * (1.0 / width)
        shifted = block - now["pivot"]
        term = lax.dot_general(
            (shifted * scale_ref[:, columns(j)]).astype(BF16), wt_ref[:, columns(j)],
            (((1,), (1,)), ((), ())), preferred_element_type=F32,
        )
        now["raw"] = term if now["raw"] is None else now["raw"] + term
        centre = jnp.sum(shifted, axis=-1, keepdims=True) * (1.0 / width)
        centred = shifted - centre
        now["centres"].append(centre)
        now["spreads"].append(jnp.sum(centred * centred, axis=-1, keepdims=True))

    step_size = step_ref[0]
    chunk_frames = (2 * FD, frames - 2 * FD)
    index = lax.broadcasted_iota(jnp.int32, (2 * FD, 1), 0)
    first_half = index < FD

    def pick(c, at):
        if c == 0:
            return jnp.where(first_half, lat_ref[: 2 * FD, at], lat_ref[frames - 2 * FD :, at])
        spread_over = pltpu.roll(
            jnp.where(first_half, lat_ref[frames - 2 * FD :, at], lat_ref[: 2 * FD, at]), FD, 0
        )
        return spread_over

    def freshen(c):
        now = state[c]
        mean = functools.reduce(jnp.add, now["centres"]) * (1.0 / n_blk)
        spread = functools.reduce(jnp.add, now["spreads"])
        for centre in now["centres"]:
            spread = spread + width * (centre - mean) * (centre - mean)
        inverse = 1.0 / jnp.sqrt(spread * (1.0 / (width * n_blk)) + EPSILON)
        flat[c][:, :channels] = inverse * (now["raw"] - mean * head_rows[:1]) + head_rows[8:9]
        for p in range(0, per_frame, 2):
            pair_of = jnp.concatenate(
                [
                    flat[c][pl.ds(p + i, chunk_frames[c], stride=per_frame), :][:, :channels]
                    for i in range(2)
                ],
                axis=1,
            )
            at = pl.ds(p * channels, 2 * channels)
            mine[c][:, at] = pick(c, at) + step_size * pair_of

    def edge_copy(slot, to):
        return pltpu.make_async_remote_copy(
            src_ref=mine[0], dst_ref=around.at[slot], send_sem=edge_send.at[0],
            recv_sem=edge_recv.at[0],
            device_id={"win": to}, device_id_type=MESH,
        )

    edges = (edge_copy(0, up_win), edge_copy(1, down_win))

    def blend():
        edge = 2 * FD
        over_prev, over_next = inter_ref[down_win], inter_ref[win]
        zero = jnp.zeros((edge, 1), jnp.int32)
        theirs_w, own_w = zero, zero
        for i in range(FD):
            hit = (index == i) & (index < over_prev)
            theirs_w = jnp.where(hit, ramps_ref[2 * i, down_win], theirs_w)
            own_w = jnp.where(hit, ramps_ref[2 * i + 1, down_win], own_w)
            hit = index == edge - over_next + i
            own_w = jnp.where(hit, ramps_ref[2 * i, win], own_w)
            theirs_w = jnp.where(hit, ramps_ref[2 * i + 1, win], theirs_w)
        aligned = jnp.zeros((edge, wide), F32)
        earlier, later = around[0], around[1]
        for o in range(1, FD + 1):
            hit = first_half & ((zero + over_prev) == o)
            aligned = jnp.where(hit, pltpu.roll(earlier, o, 0), aligned)
            hit = jnp.logical_not(first_half) & ((zero + over_next) == o)
            aligned = jnp.where(hit, pltpu.roll(later, edge - o, 0), aligned)
        theirs = theirs_w.astype(F32)
        own = jnp.where(own_w > 0, own_w, 1).astype(F32)
        mine[0][...] = (theirs * aligned + own * mine[0][...]) / (theirs + own)

    def gather_bin(i):
        c = bins[i][0][0]
        await_bytes(cross_in[c].at[: len(bins[i])], cross_recv.at[i])
        for step in bins[i]:
            gather(*step)

    gather_bin(0)
    freshen(0)
    for copy in edges:
        copy.start()
    gather_bin(1)
    gather_bin(2)
    await_bytes(around, edge_send.at[0])
    await_bytes(around, edge_recv.at[0])
    blend()
    gather_bin(3)
    gather_bin(4)
    freshen(1)

    turned = pltpu.roll(mine[1][...], FD, 0)
    out_ref[: 2 * FD, :] = jnp.where(first_half, mine[0][...], turned)
    out_ref[frames - 2 * FD :, :] = jnp.where(first_half, turned, mine[0][...])

    await_bytes(kv.at[:, :, pl.ds(0, len(peers) * rows), :], kv_send.at[0])
    await_bytes(kv.at[0, :, pl.ds(0, len(peers) * rows), :], kv_send.at[1])
    if ring:
        await_bytes(weights.at[:last], w_send.at[0])
    for c in range(2):
        await_bytes(hidden[c], part_send.at[c, 0])
        await_bytes(cross_in[c], part_send.at[c, 1])


def local(
    queries,
    keys,
    values,
    stream,
    out_weight,
    gate,
    head_shift,
    head_scale,
    head_weight,
    latents,
    step_size,
    intersections,
    ramps,
):
    rows, features = queries.shape
    groups, n_win = lax.axis_size("fsdp"), lax.axis_size("win")
    heads = features // HD // groups
    depth, part = out_weight.shape
    model = stream.shape[1]
    ring = part % 128 == 0 and n_win % 2 == 0 and n_win >= 6
    if ring:
        n_blk, width = n_win, part
    else:
        n_blk = 8
        width = model // n_blk
        out_weight = lax.all_gather(out_weight, "win", axis=1, tiled=True)
    frames, wide = latents.shape
    assert frames == 4 * FD
    channels = head_weight.shape[1]
    ends = FD * (rows // frames)
    sizes = (2 * ends, rows - 2 * ends)
    any_spec = pl.BlockSpec(memory_space=pl.ANY)
    dma = pltpu.SemaphoreType.DMA

    def both(shape, dtype):
        return tuple(pltpu.VMEM(shape(size), dtype) for size in sizes)

    parts = both(lambda size: (n_blk, size, width), BF16)
    hold = pltpu.VMEM((2 * max(sizes), width), F32)
    edge = pltpu.VMEM((2 * FD, wide), F32)
    return pl.pallas_call(
        functools.partial(kernel, ring, n_blk),
        out_shape=pltpu.VMEM(latents.shape, latents.dtype),
        in_specs=[any_spec] * 13,
        out_specs=pl.BlockSpec(memory_space=pltpu.VMEM),
        scratch_shapes=[
            pltpu.VMEM((2, heads, groups * rows, HD), BF16),
            both(lambda size: (heads, groups * size, HD), BF16),
            both(lambda size: (groups * size, heads * HD), BF16),
            pltpu.VMEM((n_blk, depth, width), BF16),
            both(lambda size: (size, model), BF16),
            hold, hold,
            parts, parts, parts, parts, parts, parts,
            both(lambda size: (n_blk, size, width), F32),
            both(lambda size: (size, 128), F32),
            (edge, pltpu.VMEM((frames - 2 * FD, wide), F32)),
            pltpu.VMEM((2, 2 * FD, wide), F32),
            pltpu.VMEM((16, channels), F32),
            pltpu.VMEM((3, rows, features), BF16),
            pltpu.VMEM((3, 1, model), F32),
            pltpu.VMEM((channels, model), head_weight.dtype),
            pltpu.VMEM((frames, wide), F32),
            pltpu.SMEM((1,), F32),
            pltpu.SMEM((n_win,), jnp.int32),
            pltpu.SMEM((2 * FD, n_win), jnp.int32),
            dma((2,)), dma((2,)), dma((heads,)), dma((heads + 1,)), dma((2,)),
            dma((1,)), dma((n_blk // 2,)), dma((1,)), dma((1,)), dma((6,)),
            dma((2, 2)), dma((2,)), dma((2,)), dma((5,)), dma((1,)), dma((1,)),
        ],
        compiler_params=pltpu.CompilerParams(
            collective_id=0, has_side_effects=True, vmem_limit_bytes=60 * 1024 * 1024
        ),
    )(
        queries, keys, values, stream, out_weight,
        gate[None, :], head_shift[None, :], head_scale[None, :], head_weight.T, latents,
        step_size, intersections, jnp.transpose(ramps, (1, 2, 0)).reshape(-1, n_win),
    )


def solution(mesh):
    in_specs = (
        P(("win", "fsdp"), None),
        P(("win", "fsdp"), None),
        P(("win", "fsdp"), None),
        P(("win", "fsdp"), None),
        P("fsdp", "win"),
        P(),
        P(),
        P(),
        P(),
        P("win", "fsdp"),
        P(),
        P(),
        P(),
    )
    out_specs = P("win", "fsdp")
    return jax.shard_map(local, mesh=mesh, in_specs=in_specs, out_specs=out_specs, check_vma=False)
```

```python
import functools
import math

import jax
import jax.numpy as jnp
from jax import lax
from jax.experimental import pallas as pl
from jax.experimental.pallas import tpu as pltpu
from jax.sharding import PartitionSpec as P

HEADS = 20
HD = 128
FD = 4
EPSILON = 0.001
MESH = pl.DeviceIdType.MESH
F32 = jnp.float32
BF16 = jnp.bfloat16


def kernel(
    ring, n_blk, q_ref, k_ref, v_ref, stream_ref, ow_ref, gate_hbm, shift_hbm, scale_hbm, wt_hbm,
    lat_hbm, step_hbm, inter_hbm, ramps_hbm, out_ref,
    kv, queries, attended, weights, residual, far_hold, near_hold, side_out, side_in, own_out,
    own_in, cross_out, cross_in, hidden, flat, mine, around, head_rows,
    staged, vectors, wt_ref, lat_ref, step_ref, inter_ref, ramps_ref, stage_sem,
    kv_send, kv_recv, q_far, own_sem, w_send, w_recv, w_local, res_sem,
    par_sem, part_send, side_recv, own_recv, cross_recv, edge_send,
    edge_recv,
):
    win, n_win = lax.axis_index("win"), lax.axis_size("win")
    me, groups = lax.axis_index("fsdp"), lax.axis_size("fsdp")
    rows = q_ref.shape[0]
    heads = kv.shape[1]
    width = weights.shape[2]
    frames, wide = lat_hbm.shape
    channels, model = wt_hbm.shape
    per_frame = rows // frames
    ends = FD * per_frame
    sizes = (2 * ends, rows - 2 * ends)
    pieces = (
        (0, 0, 0, ends),
        (0, rows - ends, ends, ends),
        (1, ends, 0, rows - 2 * ends),
    )
    chip, core = me // 2, me % 2
    sibling = chip * 2 + (1 - core)
    far_chip = 1 - chip
    far = far_chip * 2 + core
    far_sibling = far_chip * 2 + (1 - core)

    up_win, down_win = lax.rem(win + 1, n_win), lax.rem(win + n_win - 1, n_win)
    half_ring = n_win // 2

    def spot_of(w):
        odd = w % 2
        return (1 - odd) * (w // 2) + odd * (n_win - 1 - w // 2)

    def win_of(spot):
        late = spot // half_ring
        return (1 - late) * (2 * spot) + late * (2 * (n_win - 1 - spot) + 1)

    spot = spot_of(win)
    ring_next = win_of(lax.rem(spot + 1, n_win))
    ring_prev = win_of(lax.rem(spot + n_win - 1, n_win))

    if ring:
        blocks = [win]
        for s in range(1, half_ring):
            blocks.append(win_of(lax.rem(spot - s + n_win, n_win)))
            blocks.append(win_of(lax.rem(spot + s, n_win)))
        blocks.append(win_of(lax.rem(spot + half_ring, n_win)))
    else:
        blocks = [jnp.int32(j) for j in range(n_blk)]

    def columns(j):
        return pl.ds(pl.multiple_of(blocks[j] * width, 128), width)

    def head_columns(device, h):
        return pl.ds(pl.multiple_of((device * heads + h) * HD, HD), HD)

    def spots(device, size, start=0, length=None):
        length = size if length is None else length
        return pl.ds(pl.multiple_of(device * size + start, math.gcd(size, start)), length)

    peers = (far, far_sibling, sibling)
    pair = (staged.at[0], staged.at[1])
    scale_ref, shift_ref, gate_ref = (vectors.at[i] for i in range(3))

    def kv_copy(t, h, to, slot):
        return pltpu.make_async_remote_copy(
            src_ref=pair[t].at[:, head_columns(to, h)],
            dst_ref=kv.at[t, h, spots(me, rows), :],
            send_sem=kv_send.at[0],
            recv_sem=kv_recv.at[h],
            device_id={"fsdp": to},
            device_id_type=MESH,
        )

    def kv_own(t, h):
        return pltpu.make_async_copy(
            pair[t].at[:, head_columns(me, h)], kv.at[t, h, spots(me, rows), :], own_sem.at[0]
        )

    def q_copy(p, h, to, slot):
        near = slot == 2
        chunk, first, start, length = pieces[p]
        return pltpu.make_async_remote_copy(
            src_ref=staged.at[2, pl.ds(first, length), head_columns(to, h)],
            dst_ref=queries[chunk].at[h, spots(me, sizes[chunk], start, length), :],
            send_sem=kv_send.at[1],
            recv_sem=own_sem.at[1] if near else q_far.at[h if chunk == 0 else heads],
            device_id={"fsdp": to},
            device_id_type=MESH,
        )

    def q_own(p, h):
        chunk, first, start, length = pieces[p]
        return pltpu.make_async_copy(
            staged.at[2, pl.ds(first, length), head_columns(me, h)],
            queries[chunk].at[h, spots(me, sizes[chunk], start, length), :],
            own_sem.at[1],
        )

    def weight_copy(src, dst, slot, to):
        return pltpu.make_async_remote_copy(
            src_ref=src, dst_ref=dst, send_sem=w_send.at[0], recv_sem=w_recv.at[slot // 2],
            device_id={"win": to}, device_id_type=MESH,
        )

    depth_half = weights.shape[1] // 2
    last = n_blk - 1

    def forward_copies(s):
        if s < half_ring:
            up_src = ow_ref if s == 1 else weights.at[2 * s - 3]
            down_src = ow_ref if s == 1 else weights.at[2 * s - 2]
            return (
                weight_copy(up_src, weights.at[2 * s - 1], 2 * s - 2, ring_next),
                weight_copy(down_src, weights.at[2 * s], 2 * s - 1, ring_prev),
            )
        top, low = pl.ds(0, depth_half), pl.ds(depth_half, depth_half)
        return (
            weight_copy(weights.at[2 * s - 3, top], weights.at[last, top], 2 * s - 2, ring_next),
            weight_copy(weights.at[2 * s - 2, low], weights.at[last, low], 2 * s - 1, ring_prev),
        )

    def await_weights(s):
        some = weights.at[2 * s - 1 : 2 * s + 1] if s < half_ring else weights.at[last:]
        await_bytes(some, w_recv.at[s - 1])

    def weight_local(j):
        source = ow_ref if ring else ow_ref.at[:, columns(j)]
        return pltpu.make_async_copy(source, weights.at[j], w_local.at[0])

    def residual_copy(p):
        chunk, first, start, length = pieces[p]
        return pltpu.make_async_copy(
            stream_ref.at[pl.ds(first, length), :],
            residual[chunk].at[pl.ds(start, length), :],
            res_sem.at[0],
        )

    loads = [
        pltpu.make_async_copy(src, vectors.at[i], par_sem.at[0])
        for i, src in enumerate((scale_hbm, shift_hbm, gate_hbm))
    ]
    others = [
        pltpu.make_async_copy(src, dst, par_sem.at[1 + i])
        for i, (src, dst) in enumerate(
            (
                (wt_hbm, wt_ref),
                (lat_hbm, lat_ref),
                (step_hbm, step_ref),
                (inter_hbm, inter_ref),
                (ramps_hbm, ramps_ref),
            )
        )
    ]

    stages = tuple(
        pltpu.make_async_copy(src, staged.at[i], stage_sem.at[min(i, 1)])
        for i, src in enumerate((k_ref, v_ref, q_ref))
    )
    for copy in stages:
        copy.start()

    def await_bytes(like, sem):
        pltpu.make_async_copy(like, like, sem).wait()

    barrier = pltpu.get_barrier_semaphore()
    for peer in peers:
        pl.semaphore_signal(barrier, inc=1, device_id={"fsdp": peer}, device_id_type=MESH)
    greeted = [ring_next, ring_prev] if ring else [up_win, down_win]
    for other in greeted:
        pl.semaphore_signal(barrier, inc=1, device_id={"win": other}, device_id_type=MESH)
    pl.semaphore_wait(barrier, len(peers) + len(greeted))

    def start_kv(h, carry, t):
        for slot, peer in enumerate(peers):
            kv_copy(t, h, peer, slot).start()
        kv_own(t, h).start()
        return carry

    def start_q(h, carry, chosen):
        for p in chosen:
            for slot, peer in enumerate(peers):
                q_copy(p, h, peer, slot).start()
            q_own(p, h).start()
        return carry

    stages[0].wait()
    lax.fori_loop(0, heads, functools.partial(start_kv, t=0), 0)
    await_bytes(staged.at[1:], stage_sem.at[1])
    lax.fori_loop(0, heads, functools.partial(start_kv, t=1), 0)
    if ring:
        for copy in forward_copies(1):
            copy.start()
    lax.fori_loop(0, heads, functools.partial(start_q, chosen=(0, 1)), 0)
    lax.fori_loop(0, heads, functools.partial(start_q, chosen=(2,)), 0)
    for copy in loads + others:
        copy.start()
    for j in range(1 if ring else n_blk):
        weight_local(j).start()
    for p in range(len(pieces)):
        residual_copy(p).start()

    await_bytes(vectors, par_sem.at[0])
    for copy in others:
        copy.wait()
    head = wt_ref[...].astype(F32)
    for i, vector in enumerate((scale_ref, shift_ref)):
        head_rows[8 * i : 8 * i + 8] = lax.dot_general(
            jnp.broadcast_to(vector[...], (8, model)), head, (((1,), (1,)), ((), ())),
            precision=lax.Precision.HIGHEST, preferred_element_type=F32,
        )

    factor = math.log2(math.e) / math.sqrt(HD)
    def attend(h, c, at_chip):
        at = spots(at_chip, 2 * sizes[c])
        scores = lax.dot_general(
            queries[c][h, at, :], kv[0, h], (((1,), (1,)), ((), ())), preferred_element_type=F32
        )
        highest = jnp.max(scores, axis=-1, keepdims=True)
        exponent = jnp.exp2((scores - highest) * factor)
        denominator = jnp.sum(exponent, axis=-1, keepdims=True)
        summed = jnp.dot(exponent.astype(BF16), kv[1, h], preferred_element_type=F32)
        attended[c][at, pl.ds(pl.multiple_of(h * HD, HD), HD)] = (summed / denominator).astype(
            BF16
        )

    def near_head(h, carry):
        await_bytes(kv.at[:, h, pl.ds(0, len(peers) * rows), :], kv_recv.at[h])
        for c in range(2):
            attend(h, c, chip)
        return carry

    def far_head(h, carry, c):
        if c == 0:
            await_bytes(queries[c].at[h, spots(far_chip, 2 * sizes[c]), :], q_far.at[h])
        attend(h, c, far_chip)
        return carry

    own_part = pl.ds(0, rows)
    await_bytes(kv.at[:, :, own_part, :], own_sem.at[0])
    await_bytes(kv.at[:, :, own_part, :], own_sem.at[1])
    if ring:
        await_weights(1)
        for copy in forward_copies(2):
            copy.start()
    lax.fori_loop(0, heads, near_head, 0)
    lax.fori_loop(0, heads, functools.partial(far_head, c=0), 0)

    if ring:
        early = 2 * (half_ring - 2) + 1
        split = min(3, early)
        order = [(0, j) for j in range(early)] + [None] + [(1, j) for j in range(split)]
        order += [(0, j) for j in range(early, n_blk)] + [(1, j) for j in range(split, n_blk)]
    else:
        order = [(0, j) for j in range(n_blk)] + [None] + [(1, j) for j in range(n_blk)]

    steps = [step for step in order if step is not None]
    turn = {step: i for i, step in enumerate(steps)}
    a_steps = [step for step in steps if step[0] == 0]
    b_steps = [step for step in steps if step[0] == 1]
    bins = [a_steps, b_steps[:-3]] + [[step] for step in b_steps[-3:]]
    bin_of = {step: i for i, several in enumerate(bins) for step in several}

    def part_copy(src, dst, send, recv, c, j, to):
        return pltpu.make_async_remote_copy(
            src_ref=src[c].at[j], dst_ref=dst[c].at[j], send_sem=part_send.at[c, send], recv_sem=recv,
            device_id={"fsdp": to}, device_id_type=MESH,
        )

    def side_copy(c, j):
        return part_copy(side_out, side_in, 0, side_recv.at[turn[c, j] % 2], c, j, sibling)

    def own_copy(c, j):
        return part_copy(own_out, own_in, 0, own_recv.at[turn[c, j] % 2], c, j, sibling)

    def cross_copy(c, j):
        return part_copy(cross_out, cross_in, 1, cross_recv.at[bin_of[c, j]], c, j, far_sibling)

    def project(c, j):
        size = sizes[c]
        mine_at, other_at = spots(core, size), spots(1 - core, size)
        far_hold[: 2 * size] = jnp.dot(
            attended[c][spots(far_chip, 2 * size), :], weights[j], preferred_element_type=F32
        )
        side_out[c][j] = far_hold[mine_at, :].astype(BF16)
        side_copy(c, j).start()
        near_hold[: 2 * size] = jnp.dot(
            attended[c][spots(chip, 2 * size), :], weights[j], preferred_element_type=F32
        )
        own_out[c][j] = near_hold[other_at, :].astype(BF16)
        own_copy(c, j).start()
        side_copy(c, j).wait_recv()
        cross_out[c][j] = (far_hold[other_at, :] + side_in[c][j].astype(F32)).astype(BF16)
        cross_copy(c, j).start()
        own_copy(c, j).wait_recv()
        hidden[c][j] = residual[c][:, columns(j)].astype(F32) + gate_ref[:, columns(j)] * (
            near_hold[mine_at, :] + own_in[c][j].astype(F32)
        )

    await_bytes(stream_ref, res_sem.at[0])
    await_bytes(weights.at[: 1 if ring else n_blk], w_local.at[0])
    held = 1

    def advance():
        nonlocal held
        held += 1
        await_weights(held)
        if held < half_ring:
            for copy in forward_copies(held + 1):
                copy.start()

    for step in order:
        if step is None:
            far_rows = spots(far_chip, 2 * sizes[1])
            await_bytes(queries[1].at[:, far_rows, :], q_far.at[heads])
            lax.fori_loop(0, heads, functools.partial(far_head, c=1), 0)
            continue
        c, j = step
        if ring and (j + 1) // 2 > held:
            advance()
        project(c, j)
        if ring and step == steps[0]:
            advance()

    state = [dict(raw=None, pivot=None, seen=0) for _ in range(2)]

    def gather(c, j):
        now = state[c]
        block = hidden[c][j] + gate_ref[:, columns(j)] * cross_in[c][j].astype(F32)
        if now["pivot"] is None:
            now["pivot"] = jnp.sum(block, axis=-1, keepdims=True) * (1.0 / width)
        shifted = block - now["pivot"]
        term = lax.dot_general(
            (shifted * scale_ref[:, columns(j)]).astype(BF16), wt_ref[:, columns(j)],
            (((1,), (1,)), ((), ())), preferred_element_type=F32,
        )
        now["raw"] = term if now["raw"] is None else now["raw"] + term
        centre = jnp.sum(shifted, axis=-1, keepdims=True) * (1.0 / width)
        centred = shifted - centre
        spread = jnp.sum(centred * centred, axis=-1, keepdims=True)
        seen = now["seen"]
        if seen:
            apart = centre - now["mean"]
            now["mean"] += apart * (1.0 / (seen + 1))
            now["spread"] += spread + apart * apart * (width * seen / (seen + 1))
        else:
            now["mean"], now["spread"] = centre, spread
        now["seen"] = seen + 1

    step_size = step_ref[0]
    chunk_frames = (2 * FD, frames - 2 * FD)
    index = lax.broadcasted_iota(jnp.int32, (2 * FD, 1), 0)
    first_half = index < FD

    def pick(c, at):
        if c == 0:
            return jnp.where(first_half, lat_ref[: 2 * FD, at], lat_ref[frames - 2 * FD :, at])
        spread_over = pltpu.roll(
            jnp.where(first_half, lat_ref[frames - 2 * FD :, at], lat_ref[: 2 * FD, at]), FD, 0
        )
        return spread_over

    def freshen(c):
        now = state[c]
        mean, spread = now["mean"], now["spread"]
        inverse = 1.0 / jnp.sqrt(spread * (1.0 / (width * n_blk)) + EPSILON)
        flat[c][:, :channels] = inverse * (now["raw"] - mean * head_rows[:1]) + head_rows[8:9]
        for p in range(0, per_frame, 2):
            pair_of = jnp.concatenate(
                [
                    flat[c][pl.ds(p + i, chunk_frames[c], stride=per_frame), :][:, :channels]
                    for i in range(2)
                ],
                axis=1,
            )
            at = pl.ds(p * channels, 2 * channels)
            mine[c][:, at] = pick(c, at) + step_size * pair_of

    def edge_copy(slot, to):
        return pltpu.make_async_remote_copy(
            src_ref=mine[0], dst_ref=around.at[slot], send_sem=edge_send.at[0],
            recv_sem=edge_recv.at[0],
            device_id={"win": to}, device_id_type=MESH,
        )

    edges = (edge_copy(0, up_win), edge_copy(1, down_win))

    def blend():
        edge = 2 * FD
        over_prev, over_next = inter_ref[down_win], inter_ref[win]
        zero = jnp.zeros((edge, 1), jnp.int32)
        theirs_w, own_w = zero, zero
        for i in range(FD):
            hit = (index == i) & (index < over_prev)
            theirs_w = jnp.where(hit, ramps_ref[2 * i, down_win], theirs_w)
            own_w = jnp.where(hit, ramps_ref[2 * i + 1, down_win], own_w)
            hit = index == edge - over_next + i
            own_w = jnp.where(hit, ramps_ref[2 * i, win], own_w)
            theirs_w = jnp.where(hit, ramps_ref[2 * i + 1, win], theirs_w)
        aligned = jnp.zeros((edge, wide), F32)
        earlier, later = around[0], around[1]
        for o in range(1, FD + 1):
            hit = first_half & ((zero + over_prev) == o)
            aligned = jnp.where(hit, pltpu.roll(earlier, o, 0), aligned)
            hit = jnp.logical_not(first_half) & ((zero + over_next) == o)
            aligned = jnp.where(hit, pltpu.roll(later, edge - o, 0), aligned)
        theirs = theirs_w.astype(F32)
        own = jnp.where(own_w > 0, own_w, 1).astype(F32)
        mine[0][...] = (theirs * aligned + own * mine[0][...]) / (theirs + own)

    def gather_bin(i):
        c = bins[i][0][0]
        await_bytes(cross_in[c].at[: len(bins[i])], cross_recv.at[i])
        for step in bins[i]:
            gather(*step)

    gather_bin(0)
    freshen(0)
    for copy in edges:
        copy.start()
    gather_bin(1)
    gather_bin(2)
    await_bytes(around, edge_send.at[0])
    await_bytes(around, edge_recv.at[0])
    blend()
    gather_bin(3)
    gather_bin(4)
    freshen(1)

    turned = pltpu.roll(mine[1][...], FD, 0)
    out_ref[: 2 * FD, :] = jnp.where(first_half, mine[0][...], turned)
    out_ref[frames - 2 * FD :, :] = jnp.where(first_half, turned, mine[0][...])

    await_bytes(kv.at[:, :, pl.ds(0, len(peers) * rows), :], kv_send.at[0])
    await_bytes(kv.at[0, :, pl.ds(0, len(peers) * rows), :], kv_send.at[1])
    if ring:
        await_bytes(weights.at[:last], w_send.at[0])
    for c in range(2):
        await_bytes(hidden[c], part_send.at[c, 0])
        await_bytes(cross_in[c], part_send.at[c, 1])


def local(
    queries,
    keys,
    values,
    stream,
    out_weight,
    gate,
    head_shift,
    head_scale,
    head_weight,
    latents,
    step_size,
    intersections,
    ramps,
):
    rows, features = queries.shape
    groups, n_win = lax.axis_size("fsdp"), lax.axis_size("win")
    heads = features // HD // groups
    depth, part = out_weight.shape
    model = stream.shape[1]
    ring = part % 128 == 0 and n_win % 2 == 0 and n_win >= 6
    if ring:
        n_blk, width = n_win, part
    else:
        n_blk = 8
        width = model // n_blk
        out_weight = lax.all_gather(out_weight, "win", axis=1, tiled=True)
    frames, wide = latents.shape
    assert frames == 4 * FD
    channels = head_weight.shape[1]
    ends = FD * (rows // frames)
    sizes = (2 * ends, rows - 2 * ends)
    any_spec = pl.BlockSpec(memory_space=pl.ANY)
    dma = pltpu.SemaphoreType.DMA

    def both(shape, dtype):
        return tuple(pltpu.VMEM(shape(size), dtype) for size in sizes)

    parts = both(lambda size: (n_blk, size, width), BF16)
    hold = pltpu.VMEM((2 * max(sizes), width), F32)
    edge = pltpu.VMEM((2 * FD, wide), F32)
    return pl.pallas_call(
        functools.partial(kernel, ring, n_blk),
        out_shape=pltpu.VMEM(latents.shape, latents.dtype),
        in_specs=[any_spec] * 13,
        out_specs=pl.BlockSpec(memory_space=pltpu.VMEM),
        scratch_shapes=[
            pltpu.VMEM((2, heads, groups * rows, HD), BF16),
            both(lambda size: (heads, groups * size, HD), BF16),
            both(lambda size: (groups * size, heads * HD), BF16),
            pltpu.VMEM((n_blk, depth, width), BF16),
            both(lambda size: (size, model), BF16),
            hold, hold,
            parts, parts, parts, parts, parts, parts,
            both(lambda size: (n_blk, size, width), F32),
            both(lambda size: (size, 128), F32),
            (edge, pltpu.VMEM((frames - 2 * FD, wide), F32)),
            pltpu.VMEM((2, 2 * FD, wide), F32),
            pltpu.VMEM((16, channels), F32),
            pltpu.VMEM((3, rows, features), BF16),
            pltpu.VMEM((3, 1, model), F32),
            pltpu.VMEM((channels, model), head_weight.dtype),
            pltpu.VMEM((frames, wide), F32),
            pltpu.SMEM((1,), F32),
            pltpu.SMEM((n_win,), jnp.int32),
            pltpu.SMEM((2 * FD, n_win), jnp.int32),
            dma((2,)), dma((2,)), dma((heads,)), dma((heads + 1,)), dma((2,)),
            dma((1,)), dma((n_blk // 2,)), dma((1,)), dma((1,)), dma((6,)),
            dma((2, 2)), dma((2,)), dma((2,)), dma((5,)), dma((1,)), dma((1,)),
        ],
        compiler_params=pltpu.CompilerParams(
            collective_id=0, has_side_effects=True, vmem_limit_bytes=60 * 1024 * 1024
        ),
    )(
        queries, keys, values, stream, out_weight,
        gate[None, :], head_shift[None, :], head_scale[None, :], head_weight.T, latents,
        step_size, intersections, jnp.transpose(ramps, (1, 2, 0)).reshape(-1, n_win),
    )


def solution(mesh):
    in_specs = (
        P(("win", "fsdp"), None),
        P(("win", "fsdp"), None),
        P(("win", "fsdp"), None),
        P(("win", "fsdp"), None),
        P("fsdp", "win"),
        P(),
        P(),
        P(),
        P(),
        P("win", "fsdp"),
        P(),
        P(),
        P(),
    )
    out_specs = P("win", "fsdp")
    return jax.shard_map(local, mesh=mesh, in_specs=in_specs, out_specs=out_specs, check_vma=False)
```

```python
import functools
import math

import jax
import jax.numpy as jnp
from jax import lax
from jax.experimental import pallas as pl
from jax.experimental.pallas import tpu as pltpu
from jax.sharding import PartitionSpec as P

HEADS = 20
HD = 128
FD = 4
EPSILON = 0.001
MESH = pl.DeviceIdType.MESH
F32 = jnp.float32
BF16 = jnp.bfloat16


def kernel(
    ring, n_blk, q_ref, k_ref, v_ref, stream_ref, ow_ref, gate_hbm, shift_hbm, scale_hbm, wt_hbm,
    lat_hbm, step_hbm, inter_hbm, ramps_hbm, out_ref,
    kv, queries, attended, weights, residual, far_hold, near_hold, side_out, side_in, own_out,
    own_in, cross_out, cross_in, hidden, flat, mine, around, head_rows,
    staged, vectors, wt_ref, lat_ref, step_ref, inter_ref, ramps_ref, stage_sem,
    kv_send, kv_recv, q_far, own_sem, w_send, w_recv,
    part_send, side_recv, own_recv, cross_recv, edge_send,
    edge_recv,
):
    win, n_win = lax.axis_index("win"), lax.axis_size("win")
    me, groups = lax.axis_index("fsdp"), lax.axis_size("fsdp")
    rows = q_ref.shape[0]
    heads = kv.shape[1]
    width = weights.shape[2]
    frames, wide = lat_hbm.shape
    channels, model = wt_hbm.shape
    per_frame = rows // frames
    ends = FD * per_frame
    sizes = (2 * ends, rows - 2 * ends)
    pieces = (
        (0, 0, 0, ends),
        (0, rows - ends, ends, ends),
        (1, ends, 0, rows - 2 * ends),
    )
    chip, core = me // 2, me % 2
    sibling = chip * 2 + (1 - core)
    far_chip = 1 - chip
    far = far_chip * 2 + core
    far_sibling = far_chip * 2 + (1 - core)

    up_win, down_win = lax.rem(win + 1, n_win), lax.rem(win + n_win - 1, n_win)
    half_ring = n_win // 2

    def spot_of(w):
        odd = w % 2
        return (1 - odd) * (w // 2) + odd * (n_win - 1 - w // 2)

    def win_of(spot):
        late = spot // half_ring
        return (1 - late) * (2 * spot) + late * (2 * (n_win - 1 - spot) + 1)

    spot = spot_of(win)
    ring_next = win_of(lax.rem(spot + 1, n_win))
    ring_prev = win_of(lax.rem(spot + n_win - 1, n_win))

    if ring:
        blocks = [win]
        for s in range(1, half_ring):
            blocks.append(win_of(lax.rem(spot - s + n_win, n_win)))
            blocks.append(win_of(lax.rem(spot + s, n_win)))
        blocks.append(win_of(lax.rem(spot + half_ring, n_win)))
    else:
        blocks = [jnp.int32(j) for j in range(n_blk)]

    def columns(j):
        return pl.ds(pl.multiple_of(blocks[j] * width, 128), width)

    def head_columns(device, h):
        return pl.ds(pl.multiple_of((device * heads + h) * HD, HD), HD)

    def spots(device, size, start=0, length=None):
        length = size if length is None else length
        return pl.ds(pl.multiple_of(device * size + start, math.gcd(size, start)), length)

    peers = (far, far_sibling, sibling)
    pair = (staged.at[0], staged.at[1])
    scale_ref, shift_ref, gate_ref = (vectors.at[i] for i in range(3))

    def kv_copy(t, h, to, slot):
        return pltpu.make_async_remote_copy(
            src_ref=pair[t].at[:, head_columns(to, h)],
            dst_ref=kv.at[t, h, spots(me, rows), :],
            send_sem=kv_send.at[0],
            recv_sem=kv_recv.at[h // (heads - 1)],
            device_id={"fsdp": to},
            device_id_type=MESH,
        )

    def kv_own(t, h):
        return pltpu.make_async_copy(
            pair[t].at[:, head_columns(me, h)], kv.at[t, h, spots(me, rows), :], stage_sem.at[0]
        )

    def q_copy(p, h, to, slot):
        near = slot == 2
        chunk, first, start, length = pieces[p]
        return pltpu.make_async_remote_copy(
            src_ref=staged.at[2, pl.ds(first, length), head_columns(to, h)],
            dst_ref=queries[chunk].at[h, spots(me, sizes[chunk], start, length), :],
            send_sem=kv_send.at[1],
            recv_sem=own_sem.at[0] if near else q_far.at[h if chunk == 0 else heads],
            device_id={"fsdp": to},
            device_id_type=MESH,
        )

    def q_own(p, h):
        chunk, first, start, length = pieces[p]
        return pltpu.make_async_copy(
            staged.at[2, pl.ds(first, length), head_columns(me, h)],
            queries[chunk].at[h, spots(me, sizes[chunk], start, length), :],
            own_sem.at[0],
        )

    def weight_copy(src, dst, slot, to):
        return pltpu.make_async_remote_copy(
            src_ref=src, dst_ref=dst, send_sem=w_send.at[0], recv_sem=w_recv.at[slot // 2],
            device_id={"win": to}, device_id_type=MESH,
        )

    depth_half = weights.shape[1] // 2
    last = n_blk - 1

    def forward_copies(s):
        if s < half_ring:
            up_src = ow_ref if s == 1 else weights.at[2 * s - 3]
            down_src = ow_ref if s == 1 else weights.at[2 * s - 2]
            return (
                weight_copy(up_src, weights.at[2 * s - 1], 2 * s - 2, ring_next),
                weight_copy(down_src, weights.at[2 * s], 2 * s - 1, ring_prev),
            )
        top, low = pl.ds(0, depth_half), pl.ds(depth_half, depth_half)
        return (
            weight_copy(weights.at[2 * s - 3, top], weights.at[last, top], 2 * s - 2, ring_next),
            weight_copy(weights.at[2 * s - 2, low], weights.at[last, low], 2 * s - 1, ring_prev),
        )

    def await_weights(s):
        some = weights.at[2 * s - 1 : 2 * s + 1] if s < half_ring else weights.at[last:]
        await_bytes(some, w_recv.at[s - 1])

    def weight_local(j):
        source = ow_ref if ring else ow_ref.at[:, columns(j)]
        return pltpu.make_async_copy(source, weights.at[j], stage_sem.at[1])

    def residual_copy(p):
        chunk, first, start, length = pieces[p]
        return pltpu.make_async_copy(
            stream_ref.at[pl.ds(first, length), :],
            residual[chunk].at[pl.ds(start, length), :],
            stage_sem.at[1],
        )

    loads = [
        pltpu.make_async_copy(src, vectors.at[i], stage_sem.at[1])
        for i, src in enumerate((scale_hbm, shift_hbm, gate_hbm))
    ]
    others = [
        pltpu.make_async_copy(src, dst, stage_sem.at[1])
        for src, dst in (
            (wt_hbm, wt_ref),
            (lat_hbm, lat_ref),
            (step_hbm, step_ref),
            (inter_hbm, inter_ref),
            (ramps_hbm, ramps_ref),
        )
    ]

    stages = tuple(
        pltpu.make_async_copy(src, staged.at[i], stage_sem.at[min(i, 1)])
        for i, src in enumerate((k_ref, v_ref, q_ref))
    )
    for copy in stages:
        copy.start()

    def await_bytes(like, sem):
        pltpu.make_async_copy(like, like, sem).wait()

    barrier = pltpu.get_barrier_semaphore()
    for peer in peers:
        pl.semaphore_signal(barrier, inc=1, device_id={"fsdp": peer}, device_id_type=MESH)
    greeted = [ring_next, ring_prev] if ring else [up_win, down_win]
    for other in greeted:
        pl.semaphore_signal(barrier, inc=1, device_id={"win": other}, device_id_type=MESH)
    pl.semaphore_wait(barrier, len(peers) + len(greeted))

    def start_kv(h, carry, t):
        for slot, peer in enumerate(peers):
            kv_copy(t, h, peer, slot).start()
        kv_own(t, h).start()
        return carry

    def start_q(h, carry, chosen):
        for p in chosen:
            for slot, peer in enumerate(peers):
                q_copy(p, h, peer, slot).start()
            q_own(p, h).start()
        return carry

    stages[0].wait()
    lax.fori_loop(0, heads, functools.partial(start_kv, t=0), 0)
    await_bytes(staged.at[1:], stage_sem.at[1])
    lax.fori_loop(0, heads, functools.partial(start_kv, t=1), 0)
    if ring:
        for copy in forward_copies(1):
            copy.start()
    lax.fori_loop(0, heads, functools.partial(start_q, chosen=(0, 1)), 0)
    lax.fori_loop(0, heads, functools.partial(start_q, chosen=(2,)), 0)
    for copy in loads:
        copy.start()
    await_bytes(vectors, stage_sem.at[1])
    for copy in others:
        copy.start()
        copy.wait()
    for j in range(1 if ring else n_blk):
        weight_local(j).start()
    await_bytes(weights.at[: 1 if ring else n_blk], stage_sem.at[1])
    for p in range(len(pieces)):
        residual_copy(p).start()
    await_bytes(stream_ref, stage_sem.at[1])

    head = wt_ref[...].astype(F32)
    for i, vector in enumerate((scale_ref, shift_ref)):
        head_rows[8 * i : 8 * i + 8] = lax.dot_general(
            jnp.broadcast_to(vector[...], (8, model)), head, (((1,), (1,)), ((), ())),
            precision=lax.Precision.HIGHEST, preferred_element_type=F32,
        )

    factor = math.log2(math.e) / math.sqrt(HD)
    def attend(h, c, at_chip):
        at = spots(at_chip, 2 * sizes[c])
        scores = lax.dot_general(
            queries[c][h, at, :], kv[0, h], (((1,), (1,)), ((), ())), preferred_element_type=F32
        )
        highest = jnp.max(scores, axis=-1, keepdims=True)
        exponent = jnp.exp2((scores - highest) * factor)
        denominator = jnp.sum(exponent, axis=-1, keepdims=True)
        summed = jnp.dot(exponent.astype(BF16), kv[1, h], preferred_element_type=F32)
        attended[c][at, pl.ds(pl.multiple_of(h * HD, HD), HD)] = (summed / denominator).astype(
            BF16
        )

    def near_head(h, carry):
        for c in range(2):
            attend(h, c, chip)
        return carry

    def far_head(h, carry, c):
        if c == 0:
            await_bytes(queries[c].at[h, spots(far_chip, 2 * sizes[c]), :], q_far.at[h])
        attend(h, c, far_chip)
        return carry

    own_part = pl.ds(0, rows)
    await_bytes(kv.at[:, :, own_part, :], stage_sem.at[0])
    await_bytes(kv.at[:, :, own_part, :], own_sem.at[0])
    if ring:
        await_weights(1)
        for copy in forward_copies(2):
            copy.start()
    sent_part = pl.ds(0, len(peers) * rows)
    await_bytes(kv.at[:, : heads - 1, sent_part, :], kv_recv.at[0])
    lax.fori_loop(0, heads - 1, near_head, 0)
    await_bytes(kv.at[:, heads - 1, sent_part, :], kv_recv.at[1])
    near_head(heads - 1, 0)
    lax.fori_loop(0, heads, functools.partial(far_head, c=0), 0)

    if ring:
        early = 2 * (half_ring - 2) + 1
        split = min(3, early)
        order = [(0, j) for j in range(early)] + [None] + [(1, j) for j in range(split)]
        order += [(0, j) for j in range(early, n_blk)] + [(1, j) for j in range(split, n_blk)]
    else:
        order = [(0, j) for j in range(n_blk)] + [None] + [(1, j) for j in range(n_blk)]

    steps = [step for step in order if step is not None]
    turn = {step: i for i, step in enumerate(steps)}
    a_steps = [step for step in steps if step[0] == 0]
    b_steps = [step for step in steps if step[0] == 1]
    bins = [a_steps, b_steps[:-2]] + [[step] for step in b_steps[-2:]]
    cut = width - 128 if width > 128 else width
    bin_of = {step: i for i, several in enumerate(bins) for step in several}

    def part_copy(src, dst, send, recv, c, j, to):
        return pltpu.make_async_remote_copy(
            src_ref=src[c].at[j], dst_ref=dst[c].at[j], send_sem=part_send.at[c, send], recv_sem=recv,
            device_id={"fsdp": to}, device_id_type=MESH,
        )

    def side_copy(c, j):
        return part_copy(side_out, side_in, 0, side_recv.at[turn[c, j] % 2], c, j, sibling)

    def own_copy(c, j):
        return part_copy(own_out, own_in, 0, own_recv.at[turn[c, j] % 2], c, j, sibling)

    def cross_copies(c, j):
        if (c, j) != steps[-1] or cut == width:
            sem = cross_recv.at[bin_of[c, j]]
            return [part_copy(cross_out, cross_in, 1, sem, c, j, far_sibling)]
        return [
            pltpu.make_async_remote_copy(
                src_ref=cross_out[c].at[j, :, at], dst_ref=cross_in[c].at[j, :, at],
                send_sem=part_send.at[c, 1], recv_sem=cross_recv.at[3 + i],
                device_id={"fsdp": far_sibling}, device_id_type=MESH,
            )
            for i, at in enumerate((pl.ds(0, cut), pl.ds(cut, width - cut)))
        ]

    def project(c, j):
        size = sizes[c]
        mine_at, other_at = spots(core, size), spots(1 - core, size)
        far_hold[: 2 * size] = jnp.dot(
            attended[c][spots(far_chip, 2 * size), :], weights[j], preferred_element_type=F32
        )
        side_out[c][j] = far_hold[mine_at, :].astype(BF16)
        side_copy(c, j).start()
        near_hold[: 2 * size] = jnp.dot(
            attended[c][spots(chip, 2 * size), :], weights[j], preferred_element_type=F32
        )
        own_out[c][j] = near_hold[other_at, :].astype(BF16)
        own_copy(c, j).start()
        side_copy(c, j).wait_recv()
        cross_out[c][j] = (far_hold[other_at, :] + side_in[c][j].astype(F32)).astype(BF16)
        for copy in cross_copies(c, j):
            copy.start()
        own_copy(c, j).wait_recv()
        hidden[c][j] = residual[c][:, columns(j)].astype(F32) + gate_ref[:, columns(j)] * (
            near_hold[mine_at, :] + own_in[c][j].astype(F32)
        )

    held = 1

    def advance():
        nonlocal held
        held += 1
        await_weights(held)
        if held < half_ring:
            for copy in forward_copies(held + 1):
                copy.start()

    for step in order:
        if step is None:
            far_rows = spots(far_chip, 2 * sizes[1])
            await_bytes(queries[1].at[:, far_rows, :], q_far.at[heads])
            lax.fori_loop(0, heads, functools.partial(far_head, c=1), 0)
            continue
        c, j = step
        if ring and (j + 1) // 2 > held:
            advance()
        project(c, j)
        if ring and step == steps[0]:
            advance()

    state = [dict(raw=None, pivot=None, seen=0) for _ in range(2)]

    def gather(c, j, low, high):
        now = state[c]
        count = high - low
        at = pl.ds(pl.multiple_of(blocks[j] * width + low, 128), count)
        block = hidden[c][j, :, low:high] + gate_ref[:, at] * cross_in[c][j, :, low:high].astype(
            F32
        )
        if now["pivot"] is None:
            now["pivot"] = jnp.sum(block, axis=-1, keepdims=True) * (1.0 / count)
        shifted = block - now["pivot"]
        term = lax.dot_general(
            (shifted * scale_ref[:, at]).astype(BF16), wt_ref[:, at],
            (((1,), (1,)), ((), ())), preferred_element_type=F32,
        )
        now["raw"] = term if now["raw"] is None else now["raw"] + term
        centre = jnp.sum(shifted, axis=-1, keepdims=True) * (1.0 / count)
        centred = shifted - centre
        spread = jnp.sum(centred * centred, axis=-1, keepdims=True)
        seen = now["seen"]
        if seen:
            apart = centre - now["mean"]
            now["mean"] += apart * (count / (seen + count))
            now["spread"] += spread + apart * apart * (count * seen / (seen + count))
        else:
            now["mean"], now["spread"] = centre, spread
        now["seen"] = seen + count

    step_size = step_ref[0]
    chunk_frames = (2 * FD, frames - 2 * FD)
    index = lax.broadcasted_iota(jnp.int32, (2 * FD, 1), 0)
    first_half = index < FD

    def pick(c, at):
        if c == 0:
            return jnp.where(first_half, lat_ref[: 2 * FD, at], lat_ref[frames - 2 * FD :, at])
        spread_over = pltpu.roll(
            jnp.where(first_half, lat_ref[frames - 2 * FD :, at], lat_ref[: 2 * FD, at]), FD, 0
        )
        return spread_over

    def freshen(c):
        now = state[c]
        mean, spread = now["mean"], now["spread"]
        inverse = 1.0 / jnp.sqrt(spread * (1.0 / (width * n_blk)) + EPSILON)
        flat[c][:, :channels] = inverse * (now["raw"] - mean * head_rows[:1]) + head_rows[8:9]
        for p in range(0, per_frame, 2):
            pair_of = jnp.concatenate(
                [
                    flat[c][pl.ds(p + i, chunk_frames[c], stride=per_frame), :][:, :channels]
                    for i in range(2)
                ],
                axis=1,
            )
            at = pl.ds(p * channels, 2 * channels)
            mine[c][:, at] = pick(c, at) + step_size * pair_of

    def edge_copy(slot, to):
        return pltpu.make_async_remote_copy(
            src_ref=mine[0], dst_ref=around.at[slot], send_sem=edge_send.at[0],
            recv_sem=edge_recv.at[0],
            device_id={"win": to}, device_id_type=MESH,
        )

    edges = (edge_copy(0, up_win), edge_copy(1, down_win))

    def blend():
        edge = 2 * FD
        over_prev, over_next = inter_ref[down_win], inter_ref[win]
        zero = jnp.zeros((edge, 1), jnp.int32)
        theirs_w, own_w = zero, zero
        for i in range(FD):
            hit = (index == i) & (index < over_prev)
            theirs_w = jnp.where(hit, ramps_ref[2 * i, down_win], theirs_w)
            own_w = jnp.where(hit, ramps_ref[2 * i + 1, down_win], own_w)
            hit = index == edge - over_next + i
            own_w = jnp.where(hit, ramps_ref[2 * i, win], own_w)
            theirs_w = jnp.where(hit, ramps_ref[2 * i + 1, win], theirs_w)
        aligned = jnp.zeros((edge, wide), F32)
        earlier, later = around[0], around[1]
        for o in range(1, FD + 1):
            hit = first_half & ((zero + over_prev) == o)
            aligned = jnp.where(hit, pltpu.roll(earlier, o, 0), aligned)
            hit = jnp.logical_not(first_half) & ((zero + over_next) == o)
            aligned = jnp.where(hit, pltpu.roll(later, edge - o, 0), aligned)
        theirs = theirs_w.astype(F32)
        own = jnp.where(own_w > 0, own_w, 1).astype(F32)
        mine[0][...] = (theirs * aligned + own * mine[0][...]) / (theirs + own)

    def gather_bin(i):
        c = bins[i][0][0]
        await_bytes(cross_in[c].at[: len(bins[i])], cross_recv.at[i])
        for step in bins[i]:
            gather(*step, 0, width)

    gather_bin(0)
    freshen(0)
    for copy in edges:
        copy.start()
    gather_bin(1)
    await_bytes(around, edge_send.at[0])
    await_bytes(around, edge_recv.at[0])
    blend()
    gather_bin(2)
    if cut == width:
        gather_bin(3)
    else:
        for i, (low, high) in enumerate(((0, cut), (cut, width))):
            await_bytes(cross_in[1].at[steps[-1][1], :, low:high], cross_recv.at[3 + i])
            gather(*steps[-1], low, high)
    freshen(1)

    turned = pltpu.roll(mine[1][...], FD, 0)
    out_ref[: 2 * FD, :] = jnp.where(first_half, mine[0][...], turned)
    out_ref[frames - 2 * FD :, :] = jnp.where(first_half, turned, mine[0][...])

    await_bytes(kv.at[:, :, pl.ds(0, len(peers) * rows), :], kv_send.at[0])
    await_bytes(kv.at[0, :, pl.ds(0, len(peers) * rows), :], kv_send.at[1])
    if ring:
        await_bytes(weights.at[:last], w_send.at[0])
    for c in range(2):
        await_bytes(hidden[c], part_send.at[c, 0])
        await_bytes(cross_in[c], part_send.at[c, 1])


def local(
    queries,
    keys,
    values,
    stream,
    out_weight,
    gate,
    head_shift,
    head_scale,
    head_weight,
    latents,
    step_size,
    intersections,
    ramps,
):
    rows, features = queries.shape
    groups, n_win = lax.axis_size("fsdp"), lax.axis_size("win")
    heads = features // HD // groups
    depth, part = out_weight.shape
    model = stream.shape[1]
    ring = part % 128 == 0 and n_win % 2 == 0 and n_win >= 6
    if ring:
        n_blk, width = n_win, part
    else:
        n_blk = 8
        width = model // n_blk
        out_weight = lax.all_gather(out_weight, "win", axis=1, tiled=True)
    frames, wide = latents.shape
    assert frames == 4 * FD
    channels = head_weight.shape[1]
    ends = FD * (rows // frames)
    sizes = (2 * ends, rows - 2 * ends)
    any_spec = pl.BlockSpec(memory_space=pl.ANY)
    dma = pltpu.SemaphoreType.DMA

    def both(shape, dtype):
        return tuple(pltpu.VMEM(shape(size), dtype) for size in sizes)

    parts = both(lambda size: (n_blk, size, width), BF16)
    hold = pltpu.VMEM((2 * max(sizes), width), F32)
    edge = pltpu.VMEM((2 * FD, wide), F32)
    return pl.pallas_call(
        functools.partial(kernel, ring, n_blk),
        out_shape=pltpu.VMEM(latents.shape, latents.dtype),
        in_specs=[any_spec] * 13,
        out_specs=pl.BlockSpec(memory_space=pltpu.VMEM),
        scratch_shapes=[
            pltpu.VMEM((2, heads, groups * rows, HD), BF16),
            both(lambda size: (heads, groups * size, HD), BF16),
            both(lambda size: (groups * size, heads * HD), BF16),
            pltpu.VMEM((n_blk, depth, width), BF16),
            both(lambda size: (size, model), BF16),
            hold, hold,
            parts, parts, parts, parts, parts, parts,
            both(lambda size: (n_blk, size, width), F32),
            both(lambda size: (size, 128), F32),
            (edge, pltpu.VMEM((frames - 2 * FD, wide), F32)),
            pltpu.VMEM((2, 2 * FD, wide), F32),
            pltpu.VMEM((16, channels), F32),
            pltpu.VMEM((3, rows, features), BF16),
            pltpu.VMEM((3, 1, model), F32),
            pltpu.VMEM((channels, model), head_weight.dtype),
            pltpu.VMEM((frames, wide), F32),
            pltpu.SMEM((1,), F32),
            pltpu.SMEM((n_win,), jnp.int32),
            pltpu.SMEM((2 * FD, n_win), jnp.int32),
            dma((2,)), dma((2,)), dma((2,)), dma((heads + 1,)), dma((1,)),
            dma((1,)), dma((n_blk // 2,)),
            dma((2, 2)), dma((2,)), dma((2,)), dma((5,)), dma((1,)), dma((1,)),
        ],
        compiler_params=pltpu.CompilerParams(
            collective_id=0, has_side_effects=True, vmem_limit_bytes=60 * 1024 * 1024
        ),
    )(
        queries, keys, values, stream, out_weight,
        gate[None, :], head_shift[None, :], head_scale[None, :], head_weight.T, latents,
        step_size, intersections, jnp.transpose(ramps, (1, 2, 0)).reshape(-1, n_win),
    )


def solution(mesh):
    in_specs = (
        P(("win", "fsdp"), None),
        P(("win", "fsdp"), None),
        P(("win", "fsdp"), None),
        P(("win", "fsdp"), None),
        P("fsdp", "win"),
        P(),
        P(),
        P(),
        P(),
        P("win", "fsdp"),
        P(),
        P(),
        P(),
    )
    out_specs = P("win", "fsdp")
    return jax.shard_map(local, mesh=mesh, in_specs=in_specs, out_specs=out_specs, check_vma=False)
```

```python
import functools
import math

import jax
import jax.numpy as jnp
from jax import lax
from jax.experimental import pallas as pl
from jax.experimental.pallas import tpu as pltpu
from jax.sharding import PartitionSpec as P

HEADS = 20
HD = 128
FD = 4
EPSILON = 0.001
MESH = pl.DeviceIdType.MESH
F32 = jnp.float32
BF16 = jnp.bfloat16


def kernel(
    ring, n_blk, q_ref, k_ref, v_ref, stream_ref, ow_ref, gate_hbm, shift_hbm, scale_hbm, wt_hbm,
    lat_hbm, step_hbm, inter_hbm, ramps_hbm, out_ref,
    kv, queries, attended, weights, residual, far_hold, near_hold, side_out, side_in, own_out,
    own_in, cross_out, cross_in, hidden, flat, mine, around, head_rows,
    staged, vectors, wt_ref, lat_ref, step_ref, inter_ref, ramps_ref, stage_sem,
    kv_send, kv_recv, q_far, own_sem, w_send, w_recv,
    part_send, side_recv, own_recv, cross_recv, edge_send,
    edge_recv,
):
    win, n_win = lax.axis_index("win"), lax.axis_size("win")
    me, groups = lax.axis_index("fsdp"), lax.axis_size("fsdp")
    rows = q_ref.shape[0]
    heads = kv.shape[1]
    width = weights.shape[2]
    frames, wide = lat_hbm.shape
    channels, model = wt_hbm.shape
    per_frame = rows // frames
    ends = FD * per_frame
    sizes = (2 * ends, rows - 2 * ends)
    pieces = (
        (0, 0, 0, ends),
        (0, rows - ends, ends, ends),
        (1, ends, 0, rows - 2 * ends),
    )
    chip, core = me // 2, me % 2
    sibling = chip * 2 + (1 - core)
    far_chip = 1 - chip
    far = far_chip * 2 + core
    far_sibling = far_chip * 2 + (1 - core)

    up_win, down_win = lax.rem(win + 1, n_win), lax.rem(win + n_win - 1, n_win)
    half_ring = n_win // 2

    def spot_of(w):
        odd = w % 2
        return (1 - odd) * (w // 2) + odd * (n_win - 1 - w // 2)

    def win_of(spot):
        late = spot // half_ring
        return (1 - late) * (2 * spot) + late * (2 * (n_win - 1 - spot) + 1)

    spot = spot_of(win)
    ring_next = win_of(lax.rem(spot + 1, n_win))
    ring_prev = win_of(lax.rem(spot + n_win - 1, n_win))

    if ring:
        blocks = [win]
        for s in range(1, half_ring):
            blocks.append(win_of(lax.rem(spot - s + n_win, n_win)))
            blocks.append(win_of(lax.rem(spot + s, n_win)))
        blocks.append(win_of(lax.rem(spot + half_ring, n_win)))
    else:
        blocks = [jnp.int32(j) for j in range(n_blk)]

    def columns(j):
        return pl.ds(pl.multiple_of(blocks[j] * width, 128), width)

    def head_columns(device, h):
        return pl.ds(pl.multiple_of((device * heads + h) * HD, HD), HD)

    def spots(device, size, start=0, length=None):
        length = size if length is None else length
        return pl.ds(pl.multiple_of(device * size + start, math.gcd(size, start)), length)

    peers = (far, far_sibling, sibling)
    pair = (staged.at[0], staged.at[1])
    scale_ref, shift_ref, gate_ref = (vectors.at[i] for i in range(3))

    def kv_copy(t, h, to, slot):
        return pltpu.make_async_remote_copy(
            src_ref=pair[t].at[:, head_columns(to, h)],
            dst_ref=kv.at[t, h, spots(me, rows), :],
            send_sem=kv_send.at[0],
            recv_sem=kv_recv.at[h // (heads - 1)],
            device_id={"fsdp": to},
            device_id_type=MESH,
        )

    def kv_own(t, h):
        return pltpu.make_async_copy(
            pair[t].at[:, head_columns(me, h)], kv.at[t, h, spots(me, rows), :], stage_sem.at[0]
        )

    def q_copy(p, h, to, slot):
        near = slot == 2
        chunk, first, start, length = pieces[p]
        return pltpu.make_async_remote_copy(
            src_ref=staged.at[2, pl.ds(first, length), head_columns(to, h)],
            dst_ref=queries[chunk].at[h, spots(me, sizes[chunk], start, length), :],
            send_sem=kv_send.at[1],
            recv_sem=own_sem.at[0] if near else q_far.at[h if chunk == 0 else heads],
            device_id={"fsdp": to},
            device_id_type=MESH,
        )

    def q_own(p, h):
        chunk, first, start, length = pieces[p]
        return pltpu.make_async_copy(
            staged.at[2, pl.ds(first, length), head_columns(me, h)],
            queries[chunk].at[h, spots(me, sizes[chunk], start, length), :],
            own_sem.at[0],
        )

    def weight_copy(src, dst, slot, to):
        return pltpu.make_async_remote_copy(
            src_ref=src, dst_ref=dst, send_sem=w_send.at[0], recv_sem=w_recv.at[slot // 2],
            device_id={"win": to}, device_id_type=MESH,
        )

    depth_half = weights.shape[1] // 2
    last = n_blk - 1

    def forward_copies(s):
        if s < half_ring:
            up_src = ow_ref if s == 1 else weights.at[2 * s - 3]
            down_src = ow_ref if s == 1 else weights.at[2 * s - 2]
            return (
                weight_copy(up_src, weights.at[2 * s - 1], 2 * s - 2, ring_next),
                weight_copy(down_src, weights.at[2 * s], 2 * s - 1, ring_prev),
            )
        top, low = pl.ds(0, depth_half), pl.ds(depth_half, depth_half)
        return (
            weight_copy(weights.at[2 * s - 3, top], weights.at[last, top], 2 * s - 2, ring_next),
            weight_copy(weights.at[2 * s - 2, low], weights.at[last, low], 2 * s - 1, ring_prev),
        )

    def await_weights(s):
        some = weights.at[2 * s - 1 : 2 * s + 1] if s < half_ring else weights.at[last:]
        await_bytes(some, w_recv.at[s - 1])

    def weight_local(j):
        source = ow_ref if ring else ow_ref.at[:, columns(j)]
        return pltpu.make_async_copy(source, weights.at[j], stage_sem.at[1])

    def residual_copy(p):
        chunk, first, start, length = pieces[p]
        return pltpu.make_async_copy(
            stream_ref.at[pl.ds(first, length), :],
            residual[chunk].at[pl.ds(start, length), :],
            stage_sem.at[1],
        )

    loads = [
        pltpu.make_async_copy(src, vectors.at[i], stage_sem.at[1])
        for i, src in enumerate((scale_hbm, shift_hbm, gate_hbm))
    ]
    others = [
        pltpu.make_async_copy(src, dst, stage_sem.at[1])
        for src, dst in (
            (wt_hbm, wt_ref),
            (lat_hbm, lat_ref),
            (step_hbm, step_ref),
            (inter_hbm, inter_ref),
            (ramps_hbm, ramps_ref),
        )
    ]

    stages = tuple(
        pltpu.make_async_copy(src, staged.at[i], stage_sem.at[min(i, 1)])
        for i, src in enumerate((k_ref, v_ref, q_ref))
    )
    for copy in stages:
        copy.start()

    def await_bytes(like, sem):
        pltpu.make_async_copy(like, like, sem).wait()

    barrier = pltpu.get_barrier_semaphore()
    for peer in peers:
        pl.semaphore_signal(barrier, inc=1, device_id={"fsdp": peer}, device_id_type=MESH)
    greeted = [ring_next, ring_prev] if ring else [up_win, down_win]
    for other in greeted:
        pl.semaphore_signal(barrier, inc=1, device_id={"win": other}, device_id_type=MESH)
    pl.semaphore_wait(barrier, len(peers) + len(greeted))

    def start_kv(h, carry, t):
        for slot, peer in enumerate(peers):
            kv_copy(t, h, peer, slot).start()
        kv_own(t, h).start()
        return carry

    def start_q(h, carry, chosen):
        for p in chosen:
            for slot, peer in enumerate(peers):
                q_copy(p, h, peer, slot).start()
            q_own(p, h).start()
        return carry

    stages[0].wait()
    lax.fori_loop(0, heads, functools.partial(start_kv, t=0), 0)
    await_bytes(staged.at[1:], stage_sem.at[1])
    lax.fori_loop(0, heads, functools.partial(start_kv, t=1), 0)
    if ring:
        for copy in forward_copies(1):
            copy.start()
    lax.fori_loop(0, heads, functools.partial(start_q, chosen=(0, 1)), 0)
    lax.fori_loop(0, heads, functools.partial(start_q, chosen=(2,)), 0)
    for copy in loads:
        copy.start()
    await_bytes(vectors, stage_sem.at[1])
    for copy in others:
        copy.start()
        copy.wait()
    for j in range(1 if ring else n_blk):
        weight_local(j).start()
    await_bytes(weights.at[: 1 if ring else n_blk], stage_sem.at[1])
    for p in range(len(pieces)):
        residual_copy(p).start()
    await_bytes(stream_ref, stage_sem.at[1])

    head = wt_ref[...].astype(F32)
    for i, vector in enumerate((scale_ref, shift_ref)):
        head_rows[8 * i : 8 * i + 8] = lax.dot_general(
            jnp.broadcast_to(vector[...], (8, model)), head, (((1,), (1,)), ((), ())),
            precision=lax.Precision.HIGHEST, preferred_element_type=F32,
        )

    factor = math.log2(math.e) / math.sqrt(HD)
    def attend(h, c, at_chip):
        at = spots(at_chip, 2 * sizes[c])
        scores = lax.dot_general(
            queries[c][h, at, :], kv[0, h], (((1,), (1,)), ((), ())), preferred_element_type=F32
        )
        highest = jnp.max(scores, axis=-1, keepdims=True)
        exponent = jnp.exp2((scores - highest) * factor)
        denominator = jnp.sum(exponent, axis=-1, keepdims=True)
        summed = jnp.dot(exponent.astype(BF16), kv[1, h], preferred_element_type=F32)
        attended[c][at, pl.ds(pl.multiple_of(h * HD, HD), HD)] = (summed / denominator).astype(
            BF16
        )

    def near_head(h, carry):
        for c in range(2):
            attend(h, c, chip)
        return carry

    def far_head(h, carry, c):
        if c == 0:
            await_bytes(queries[c].at[h, spots(far_chip, 2 * sizes[c]), :], q_far.at[h])
        attend(h, c, far_chip)
        return carry

    own_part = pl.ds(0, rows)
    await_bytes(kv.at[:, :, own_part, :], stage_sem.at[0])
    await_bytes(kv.at[:, :, own_part, :], own_sem.at[0])
    if ring:
        await_weights(1)
        for copy in forward_copies(2):
            copy.start()
    sent_part = pl.ds(0, len(peers) * rows)
    await_bytes(kv.at[:, : heads - 1, sent_part, :], kv_recv.at[0])
    lax.fori_loop(0, heads - 1, near_head, 0)
    await_bytes(kv.at[:, heads - 1, sent_part, :], kv_recv.at[1])
    near_head(heads - 1, 0)
    lax.fori_loop(0, heads, functools.partial(far_head, c=0), 0)

    if ring:
        early = 2 * (half_ring - 2) + 1
        split = min(3, early)
        order = [(0, j) for j in range(early)] + [None] + [(1, j) for j in range(split)]
        order += [(0, j) for j in range(early, n_blk)] + [(1, j) for j in range(split, n_blk)]
    else:
        order = [(0, j) for j in range(n_blk)] + [None] + [(1, j) for j in range(n_blk)]

    steps = [step for step in order if step is not None]
    turn = {step: i for i, step in enumerate(steps)}
    a_steps = [step for step in steps if step[0] == 0]
    b_steps = [step for step in steps if step[0] == 1]
    bins = [a_steps, b_steps[:-2]] + [[step] for step in b_steps[-2:]]
    cut = width - 128 if width > 128 else width
    bin_of = {step: i for i, several in enumerate(bins) for step in several}

    def part_copy(src, dst, send, recv, c, j, to):
        return pltpu.make_async_remote_copy(
            src_ref=src[c].at[j], dst_ref=dst[c].at[j], send_sem=part_send.at[c, send], recv_sem=recv,
            device_id={"fsdp": to}, device_id_type=MESH,
        )

    def side_copy(c, j):
        return part_copy(side_out, side_in, 0, side_recv.at[turn[c, j] % 2], c, j, sibling)

    def own_copy(c, j):
        return part_copy(own_out, own_in, 0, own_recv.at[turn[c, j] % 2], c, j, sibling)

    def cross_copies(c, j):
        if (c, j) != steps[-1] or cut == width:
            sem = cross_recv.at[bin_of[c, j]]
            return [part_copy(cross_out, cross_in, 1, sem, c, j, far_sibling)]
        return [
            pltpu.make_async_remote_copy(
                src_ref=cross_out[c].at[j, :, at], dst_ref=cross_in[c].at[j, :, at],
                send_sem=part_send.at[c, 1], recv_sem=cross_recv.at[3 + i],
                device_id={"fsdp": far_sibling}, device_id_type=MESH,
            )
            for i, at in enumerate((pl.ds(0, cut), pl.ds(cut, width - cut)))
        ]

    def project(c, j):
        size = sizes[c]
        mine_at, other_at = spots(core, size), spots(1 - core, size)
        far_hold[: 2 * size] = jnp.dot(
            attended[c][spots(far_chip, 2 * size), :], weights[j], preferred_element_type=F32
        )
        side_out[c][j] = far_hold[mine_at, :].astype(BF16)
        side_copy(c, j).start()
        near_hold[: 2 * size] = jnp.dot(
            attended[c][spots(chip, 2 * size), :], weights[j], preferred_element_type=F32
        )
        own_out[c][j] = near_hold[other_at, :].astype(BF16)
        own_copy(c, j).start()
        side_copy(c, j).wait_recv()
        cross_out[c][j] = (far_hold[other_at, :] + side_in[c][j].astype(F32)).astype(BF16)
        for copy in cross_copies(c, j):
            copy.start()
        own_copy(c, j).wait_recv()
        hidden[c][j] = residual[c][:, columns(j)].astype(F32) + gate_ref[:, columns(j)] * (
            near_hold[mine_at, :] + own_in[c][j].astype(F32)
        )

    held = 1

    def advance():
        nonlocal held
        held += 1
        await_weights(held)
        if held < half_ring:
            for copy in forward_copies(held + 1):
                copy.start()

    for step in order:
        if step is None:
            far_rows = spots(far_chip, 2 * sizes[1])
            await_bytes(queries[1].at[:, far_rows, :], q_far.at[heads])
            lax.fori_loop(0, heads, functools.partial(far_head, c=1), 0)
            continue
        c, j = step
        if ring and (j + 1) // 2 > held:
            advance()
        project(c, j)
        if ring and step == steps[0]:
            advance()

    state = [dict(raw=None, pivot=None, seen=0) for _ in range(2)]

    def gather(c, j, low, high):
        now = state[c]
        count = high - low
        at = pl.ds(pl.multiple_of(blocks[j] * width + low, 128), count)
        block = hidden[c][j, :, low:high] + gate_ref[:, at] * cross_in[c][j, :, low:high].astype(
            F32
        )
        if now["pivot"] is None:
            now["pivot"] = jnp.sum(block, axis=-1, keepdims=True) * (1.0 / count)
        shifted = block - now["pivot"]
        term = lax.dot_general(
            (shifted * scale_ref[:, at]).astype(BF16), wt_ref[:, at],
            (((1,), (1,)), ((), ())), preferred_element_type=F32,
        )
        now["raw"] = term if now["raw"] is None else now["raw"] + term
        centre = jnp.sum(shifted, axis=-1, keepdims=True) * (1.0 / count)
        centred = shifted - centre
        spread = jnp.sum(centred * centred, axis=-1, keepdims=True)
        seen = now["seen"]
        if seen:
            apart = centre - now["mean"]
            now["mean"] += apart * (count / (seen + count))
            now["spread"] += spread + apart * apart * (count * seen / (seen + count))
        else:
            now["mean"], now["spread"] = centre, spread
        now["seen"] = seen + count

    step_size = step_ref[0]
    chunk_frames = (2 * FD, frames - 2 * FD)
    index = lax.broadcasted_iota(jnp.int32, (2 * FD, 1), 0)
    first_half = index < FD

    def freshen(c):
        now = state[c]
        mean, spread = now["mean"], now["spread"]
        inverse = 1.0 / jnp.sqrt(spread * (1.0 / (width * n_blk)) + EPSILON)
        flat[c][:, :channels] = inverse * (now["raw"] - mean * head_rows[:1]) + head_rows[8:9]
        for p in range(0, per_frame, 2):
            pair_of = jnp.concatenate(
                [
                    flat[c][pl.ds(p + i, chunk_frames[c], stride=per_frame), :][:, :channels]
                    for i in range(2)
                ],
                axis=1,
            )
            at = pl.ds(p * channels, 2 * channels)
            if c == 0:
                start = jnp.where(first_half, lat_ref[: 2 * FD, at], lat_ref[2 * FD :, at])
                mine[:, at] = start + step_size * pair_of
            else:
                turned = pltpu.roll(step_size * pair_of, FD, 0)
                out_ref[: 2 * FD, at] += jnp.where(first_half, 0.0, turned)
                out_ref[2 * FD :, at] += jnp.where(first_half, turned, 0.0)

    def edge_copy(slot, to):
        return pltpu.make_async_remote_copy(
            src_ref=mine, dst_ref=around.at[slot], send_sem=edge_send.at[0],
            recv_sem=edge_recv.at[0],
            device_id={"win": to}, device_id_type=MESH,
        )

    edges = (edge_copy(0, up_win), edge_copy(1, down_win))

    def blend():
        edge = 2 * FD
        over_prev, over_next = inter_ref[down_win], inter_ref[win]
        zero = jnp.zeros((edge, 1), jnp.int32)
        theirs_w, own_w = zero, zero
        for i in range(FD):
            hit = (index == i) & (index < over_prev)
            theirs_w = jnp.where(hit, ramps_ref[2 * i, down_win], theirs_w)
            own_w = jnp.where(hit, ramps_ref[2 * i + 1, down_win], own_w)
            hit = index == edge - over_next + i
            own_w = jnp.where(hit, ramps_ref[2 * i, win], own_w)
            theirs_w = jnp.where(hit, ramps_ref[2 * i + 1, win], theirs_w)
        aligned = jnp.zeros((edge, wide), F32)
        earlier, later = around[0], around[1]
        for o in range(1, FD + 1):
            hit = first_half & ((zero + over_prev) == o)
            aligned = jnp.where(hit, pltpu.roll(earlier, o, 0), aligned)
            hit = jnp.logical_not(first_half) & ((zero + over_next) == o)
            aligned = jnp.where(hit, pltpu.roll(later, edge - o, 0), aligned)
        theirs = theirs_w.astype(F32)
        own = jnp.where(own_w > 0, own_w, 1).astype(F32)
        mine[...] = (theirs * aligned + own * mine[...]) / (theirs + own)

    def gather_bin(i):
        c = bins[i][0][0]
        await_bytes(cross_in[c].at[: len(bins[i])], cross_recv.at[i])
        for step in bins[i]:
            gather(*step, 0, width)

    gather_bin(0)
    freshen(0)
    for copy in edges:
        copy.start()
    gather_bin(1)
    await_bytes(around, edge_send.at[0])
    await_bytes(around, edge_recv.at[0])
    blend()
    out_ref[: 2 * FD, :] = jnp.where(first_half, mine[...], lat_ref[: 2 * FD, :])
    out_ref[2 * FD :, :] = jnp.where(first_half, lat_ref[2 * FD :, :], mine[...])
    gather_bin(2)
    if cut == width:
        gather_bin(3)
    else:
        for i, (low, high) in enumerate(((0, cut), (cut, width))):
            await_bytes(cross_in[1].at[steps[-1][1], :, low:high], cross_recv.at[3 + i])
            gather(*steps[-1], low, high)
    freshen(1)

    await_bytes(kv.at[:, :, pl.ds(0, len(peers) * rows), :], kv_send.at[0])
    await_bytes(kv.at[0, :, pl.ds(0, len(peers) * rows), :], kv_send.at[1])
    if ring:
        await_bytes(weights.at[:last], w_send.at[0])
    for c in range(2):
        await_bytes(hidden[c], part_send.at[c, 0])
        await_bytes(cross_in[c], part_send.at[c, 1])


def local(
    queries,
    keys,
    values,
    stream,
    out_weight,
    gate,
    head_shift,
    head_scale,
    head_weight,
    latents,
    step_size,
    intersections,
    ramps,
):
    rows, features = queries.shape
    groups, n_win = lax.axis_size("fsdp"), lax.axis_size("win")
    heads = features // HD // groups
    depth, part = out_weight.shape
    model = stream.shape[1]
    ring = part % 128 == 0 and n_win % 2 == 0 and n_win >= 6
    if ring:
        n_blk, width = n_win, part
    else:
        n_blk = 8
        width = model // n_blk
        out_weight = lax.all_gather(out_weight, "win", axis=1, tiled=True)
    frames, wide = latents.shape
    assert frames == 4 * FD
    channels = head_weight.shape[1]
    ends = FD * (rows // frames)
    sizes = (2 * ends, rows - 2 * ends)
    any_spec = pl.BlockSpec(memory_space=pl.ANY)
    dma = pltpu.SemaphoreType.DMA

    def both(shape, dtype):
        return tuple(pltpu.VMEM(shape(size), dtype) for size in sizes)

    parts = both(lambda size: (n_blk, size, width), BF16)
    hold = pltpu.VMEM((2 * max(sizes), width), F32)
    edge = pltpu.VMEM((2 * FD, wide), F32)
    return pl.pallas_call(
        functools.partial(kernel, ring, n_blk),
        out_shape=pltpu.VMEM(latents.shape, latents.dtype),
        in_specs=[any_spec] * 13,
        out_specs=pl.BlockSpec(memory_space=pltpu.VMEM),
        scratch_shapes=[
            pltpu.VMEM((2, heads, groups * rows, HD), BF16),
            both(lambda size: (heads, groups * size, HD), BF16),
            both(lambda size: (groups * size, heads * HD), BF16),
            pltpu.VMEM((n_blk, depth, width), BF16),
            both(lambda size: (size, model), BF16),
            hold, hold,
            parts, parts, parts, parts, parts, parts,
            both(lambda size: (n_blk, size, width), F32),
            both(lambda size: (size, 128), F32),
            edge,
            pltpu.VMEM((2, 2 * FD, wide), F32),
            pltpu.VMEM((16, channels), F32),
            pltpu.VMEM((3, rows, features), BF16),
            pltpu.VMEM((3, 1, model), F32),
            pltpu.VMEM((channels, model), head_weight.dtype),
            pltpu.VMEM((frames, wide), F32),
            pltpu.SMEM((1,), F32),
            pltpu.SMEM((n_win,), jnp.int32),
            pltpu.SMEM((2 * FD, n_win), jnp.int32),
            dma((2,)), dma((2,)), dma((2,)), dma((heads + 1,)), dma((1,)),
            dma((1,)), dma((n_blk // 2,)),
            dma((2, 2)), dma((2,)), dma((2,)), dma((5,)), dma((1,)), dma((1,)),
        ],
        compiler_params=pltpu.CompilerParams(
            collective_id=0, has_side_effects=True, vmem_limit_bytes=60 * 1024 * 1024
        ),
    )(
        queries, keys, values, stream, out_weight,
        gate[None, :], head_shift[None, :], head_scale[None, :], head_weight.T, latents,
        step_size, intersections, jnp.transpose(ramps, (1, 2, 0)).reshape(-1, n_win),
    )


def solution(mesh):
    in_specs = (
        P(("win", "fsdp"), None),
        P(("win", "fsdp"), None),
        P(("win", "fsdp"), None),
        P(("win", "fsdp"), None),
        P("fsdp", "win"),
        P(),
        P(),
        P(),
        P(),
        P("win", "fsdp"),
        P(),
        P(),
        P(),
    )
    out_specs = P("win", "fsdp")
    return jax.shard_map(local, mesh=mesh, in_specs=in_specs, out_specs=out_specs, check_vma=False)
```
